128 devices in a mesh: gx: 4 (over x), gy: 8 (over y, core), gz: 4 (over z).
Axes of the slice: x: 4, y: 4, z: 4, core: 2. Of those that a mesh axis runs over, the one named last changes fastest.
Arguments:
- labels: int32 [128, 512, 512], P('gx', 'gy', 'gz'), may hold values from 0 to 7
- conductivity: float32 [7, 8], replicated, may hold values from -0.08 to 2, as said below
- right_side: float32 [128, 512, 512], P('gx', 'gy', 'gz'), may hold values from -18 to 18
Outputs:
- solution: float32 [128, 512, 512], P('gx', 'gy', 'gz')
The draws below stay inside these ranges and needn't reach their ends.
Inputs may be any that keep to these rules, and one draw needn't show every extreme that they name: `conductivity`: rows 0 to 2 are positive, rows 3 to 5 have magnitude at most 0.08, row 6 is at least 0.5.
All inputs are finite; a program needn't handle non-finite values.
Results may differ from the reference program's by a relative error of at most 0.0001.
Values sent between devices are 32-bit elements; how exact they have to be, the bound alone decides.
No kernel may reach another device: no remote copies, remote signals or barrier semaphores. Data moves between devices by JAX's collectives and lax.ppermute only.
A program may use at most 128 MiB of HBM per device.

```python
import math
import jax
import jax.numpy as jnp
from jax import lax

ITERS = 3
LABELS = 8
NX = 128
NY = 512
NZ = 512


def draw_conductivity(key, part):
    key_diag = jax.random.fold_in(key, 11)
    key_off = jax.random.fold_in(key, 12)
    key_mass = jax.random.fold_in(key, 13)
    diagonal = jnp.exp(jax.random.uniform(key_diag, (3, LABELS), jnp.float32, math.log(0.5), math.log(2.0)))
    offdiag = jax.random.uniform(key_off, (3, LABELS), jnp.float32, -0.08, 0.08)
    mass = jnp.exp(jax.random.uniform(key_mass, (1, LABELS), jnp.float32, math.log(0.5), math.log(1.0)))
    return jnp.concatenate([diagonal, offdiag, mass], axis=0).astype(jnp.float32)


def draw_right_side(key, part):
    key_base = jax.random.fold_in(key, 21)
    key_scale = jax.random.fold_in(key, 22)
    column = jnp.exp(jax.random.uniform(key_scale, (NX, NY, 1), jnp.float32, math.log(0.3), math.log(3.0)))
    ramp = 0.5 + jnp.arange(NY, dtype=jnp.float32)[None, :, None] / NY
    base = jnp.clip(jax.random.normal(key_base, (NX, NY, NZ), jnp.float32), -3.6, 3.6)
    return (base * column * ramp + 1.0).astype(jnp.float32)


def place_ends(array, stream_key, low, top_value):
    index_at = [jax.random.randint(jax.random.fold_in(stream_key, axis), (), 0, length) for axis, length in enumerate(array.shape)]
    widest = array.shape.index(max(array.shape))
    neighbour = index_at[:widest] + [(index_at[widest] + 1) % array.shape[widest]] + index_at[widest + 1:]
    return array.at[tuple(index_at)].set(low).at[tuple(neighbour)].set(top_value)


def setup_inputs(seed: int = 0) -> dict:
    arg_keys = jax.random.split(jax.random.key(seed), 4)
    labels = place_ends(jax.random.randint(arg_keys[0], (NX, NY, NZ), 0, LABELS), jax.random.fold_in(arg_keys[0], 1), 0, LABELS - 1).astype(jnp.int32)
    conductivity = draw_conductivity(jax.random.fold_in(arg_keys[3], 71), 0)
    right_side = draw_right_side(jax.random.fold_in(arg_keys[3], 71), 0)
    return {"labels": labels, "conductivity": conductivity, "right_side": right_side}


def neighbour_value(arr, shift_x, shift_y, shift_z, cell_grid):
    size_x, size_y, size_z = cell_grid
    return arr[..., 1 + shift_x:1 + shift_x + size_x, 1 + shift_y:1 + shift_y + size_y, 1 + shift_z:1 + shift_z + size_z]


def stencil_apply(padded_value, padded_sigma, self_coefficient):
    cell_grid = self_coefficient.shape
    value_entry = neighbour_value(padded_value, 0, 0, 0, cell_grid)
    total_flux = self_coefficient * value_entry
    for axis in range(3):
        for sign in (-1, 1):
            stencil_offset = [0, 0, 0]
            stencil_offset[axis] = sign
            face_flux = 0.5 * (neighbour_value(padded_sigma[axis], 0, 0, 0, cell_grid) + neighbour_value(padded_sigma[axis], stencil_offset[0], stencil_offset[1], stencil_offset[2], cell_grid))
            total_flux = total_flux + face_flux * (value_entry - neighbour_value(padded_value, stencil_offset[0], stencil_offset[1], stencil_offset[2], cell_grid))
    for first, second, comp in ((0, 1, 3), (0, 2, 4), (1, 2, 5)):
        for sign_a in (-1, 1):
            for sign_b in (-1, 1):
                stencil_offset = [0, 0, 0]
                stencil_offset[first] = sign_a
                stencil_offset[second] = sign_b
                cross_term = (0.25 * sign_a * sign_b) * (neighbour_value(padded_sigma[comp], 0, 0, 0, cell_grid) + neighbour_value(padded_sigma[comp], stencil_offset[0], stencil_offset[1], stencil_offset[2], cell_grid))
                total_flux = total_flux - cross_term * neighbour_value(padded_value, stencil_offset[0], stencil_offset[1], stencil_offset[2], cell_grid)
    return total_flux


def diagonal_of(padded_sigma, self_coefficient):
    cell_grid = self_coefficient.shape
    total_flux = self_coefficient
    for axis in range(3):
        for sign in (-1, 1):
            stencil_offset = [0, 0, 0]
            stencil_offset[axis] = sign
            total_flux = total_flux + 0.5 * (neighbour_value(padded_sigma[axis], 0, 0, 0, cell_grid) + neighbour_value(padded_sigma[axis], stencil_offset[0], stencil_offset[1], stencil_offset[2], cell_grid))
    return total_flux


def reference(labels, conductivity, right_side):
    extended = jnp.concatenate([jnp.zeros((7, 1), conductivity.dtype), conductivity], axis=1)
    label_pad = jnp.pad(labels.astype(jnp.int32) + 1, 1)
    planes = jnp.arange(labels.shape[0], dtype=jnp.int32)

    def slab_table(index):
        part = lax.dynamic_slice_in_dim(label_pad, index, 3, 0)
        table = jnp.take(extended, part, axis=1)
        return table[:6], table[6, 1:2, 1:-1, 1:-1]

    def diag_plane(index):
        padded_sigma, self_coefficient = slab_table(index)
        return diagonal_of(padded_sigma, self_coefficient)[0]

    diag = lax.map(diag_plane, planes)

    def operate(field):
        field_pad = jnp.pad(field, 1)

        def one_plane(index):
            padded_sigma, self_coefficient = slab_table(index)
            part = lax.dynamic_slice_in_dim(field_pad, index, 3, 0)
            return stencil_apply(part, padded_sigma, self_coefficient)[0]

        return lax.map(one_plane, planes)

    solution = jnp.zeros_like(right_side)
    residual = right_side
    precond = residual / diag
    direction = precond
    gamma = jnp.sum(residual * precond)
    for step in range(ITERS):
        image = operate(direction)
        alpha = gamma / jnp.sum(direction * image)
        solution = solution + alpha * direction
        residual = residual - alpha * image
        precond = residual / diag
        fresh = jnp.sum(residual * precond)
        direction = precond + (fresh / gamma) * direction
        gamma = fresh
    return solution
```

```python
import jax
import jax.numpy as jnp
from jax import lax
from jax.experimental import pallas as pl
from jax.experimental.pallas import tpu as pltpu
from jax.sharding import PartitionSpec as P

LABELS = 8
ALL = ("gx", "gy", "gz")
NX, NY, NZ = 32, 64, 128
XP, RW = NX + 8, NY + 16
OWN = slice(8, 8 + NY)
F32 = jnp.float32


def ring(arr, axis, step):
    count = lax.axis_size(axis)
    return lax.ppermute(arr, axis, [(i, (i + step) % count) for i in range(count)])


def iota(shape, dim):
    return lax.broadcasted_iota(jnp.int32, shape, dim)


def pack_rows(lab0, lab7, b0, b7, xu0, xu7, xl0, xl7, up, down):
    low = iota((8, 128), 0) < 4

    def put(xp, lab_first, lab_last, b_first, b_last):
        up[xp] = jnp.where(low, b_first, pltpu.roll(lab_first, 4, 0))
        down[xp] = jnp.where(low, pltpu.roll(lab_last, 4, 0), b_last)

    def own(x, carry):
        put(x + 4, lab0[x].astype(F32), lab7[x].astype(F32), b0[x], b7[x])
        return carry

    lax.fori_loop(0, NX, own, 0)
    zero = jnp.zeros((8, 128), F32)
    for k in range(4):
        bk = (xl0[k - 1], xl7[k - 1]) if k else (zero, zero)
        put(k, xl0[3 + k], xl7[3 + k], *bk)
        bk = (xu0[k], xu7[k]) if k < 3 else (zero, zero)
        put(36 + k, xu0[3 + k], xu7[3 + k], *bk)


def rows_lab(yu, yd, xp):
    low = iota((8, 128), 0) < 4
    return pltpu.roll(jnp.where(low, yd[xp], yu[xp]), 4, 0)


def rows_b(yu, yd, xp):
    low = iota((8, 128), 0) < 4
    return jnp.where(low, yu[xp], yd[xp])


def pack_lanes(lab, b, xu, xl, yu, yd, up, down, acc_lab, acc_b):
    group = iota((RW, 128), 1) // 8

    def put(xp, lab_own, b_own):
        k = xp % 16
        g = xp // 16
        lab8 = rows_lab(yu, yd, xp)
        b8 = rows_b(yu, yd, xp)
        hit = group == k
        shift = 8 * k + 4
        full = jnp.concatenate([lab8, lab_own, lab8], 0)
        acc_lab[g] = jnp.where(hit, pltpu.roll(full, shift, 1), acc_lab[g])
        full = jnp.concatenate([b8, b_own, b8], 0)
        acc_b[g] = jnp.where(hit, pltpu.roll(full, shift, 1), acc_b[g])

    acc_lab[...] = jnp.zeros((3, RW, 128), F32)
    acc_b[...] = jnp.zeros((3, RW, 128), F32)

    def own(x, carry):
        put(x + 4, lab[x].astype(F32), b[x])
        return carry

    lax.fori_loop(0, NX, own, 0)
    zero = jnp.zeros((NY, 128), F32)
    for k in range(4):
        put(k, xl[3 + k], xl[k - 1] if k else zero)
        put(36 + k, xu[3 + k], xu[k] if k < 3 else zero)
    first = iota((RW, 128), 1) % 8 < 4
    for g in range(3):
        down[g] = jnp.where(first, acc_lab[g], pltpu.roll(acc_b[g], 4, 1))
        up[g] = jnp.where(first, pltpu.roll(acc_b[g], 124, 1), acc_lab[g])


def sweeps(
    cond, lab, b, xu, xl, yu, yd, zu_own, zd_own, zu, zd,
    w0o, w1o, w2o, mom,
    s0, s1, s2, s3, s4, s5, inv, mid, v0, v1, v2, dz, ac, u3, u4, u5,
    q0, q1, q2, q3, q4, q5, qinv, qmid, qv0, qv1, qv2, qdz, qac, p3, p4, p5,
    wide, patch_v, patch_q, row_v, row_q,
):
    sig = (s0, s1, s2, s3, s4, s5)
    qsig = (q0, q1, q2, q3, q4, q5)
    gx, gy, gz = (lax.axis_index(a) for a in ALL)
    not_first_x = (gx > 0).astype(F32)
    not_last_x = (gx < lax.axis_size("gx") - 1).astype(F32)
    not_first_y = (gy > 0).astype(F32)
    not_last_y = (gy < lax.axis_size("gy") - 1).astype(F32)
    not_first_z = (gz > 0).astype(F32)
    not_last_z = (gz < lax.axis_size("gz") - 1).astype(F32)

    sub8 = iota((8, 128), 0)
    tables = []
    for c in range(7):
        t = jnp.zeros((8, 128), F32)
        scale = 0.5 if c < 3 else (0.25 if c < 6 else 1.0)
        for l in range(LABELS):
            t = jnp.where(sub8 == l, cond[c, l] * scale, t)
        tables.append(t)

    mass = sum(cond[6, l] for l in range(LABELS))
    faces = sum(cond[c, l] for c in range(3) for l in range(LABELS)) * 2.0
    theta = jnp.full((1, 128), faces, F32) / jnp.full((1, 128), faces + mass, F32)

    def look(c, idx):
        return jnp.take_along_axis(tables[c], idx, axis=0, mode="promise_in_bounds")

    def entries(idx, on):
        vals = [look(c, idx) for c in range(7)]
        if on is not None:
            vals = [v * on for v in vals]
        centre = vals[6] + 2.0 * (vals[0] + vals[1] + vals[2])
        return vals[:6], centre

    row_on = jnp.where(sub8 < 4, not_last_y, not_first_y)

    def table_plane(xp, labels_of, b_own, on):
        for g in range(8):
            vals, centre = entries(labels_of(g), on)
            at = pl.ds(8 + 8 * g, 8)
            for c in range(6):
                sig[c][xp, at] = vals[c]
            inv[xp, at] = centre
        vals, centre = entries(
            rows_lab(yu, yd, xp).astype(jnp.int32), row_on if on is None else row_on * on
        )
        b8 = rows_b(yu, yd, xp)
        for at in (pl.ds(0, 8), pl.ds(72, 8)):
            for c in range(6):
                sig[c][xp, at] = vals[c]
            inv[xp, at] = centre
            v0[xp, at] = b8
        v0[xp, OWN] = b_own

    def own_plane(x, carry):
        table_plane(x + 4, lambda g: lab[x, pl.ds(8 * g, 8)], b[x], None)
        return carry

    lax.fori_loop(0, NX, own_plane, 0)
    zero = jnp.zeros((NY, 128), F32)

    def low_plane(k, carry):
        table_plane(
            k,
            lambda g: xl[3 + k, pl.ds(8 * g, 8)].astype(jnp.int32),
            xl[jnp.maximum(k - 1, 0)],
            not_first_x,
        )
        return carry

    def high_plane(k, carry):
        table_plane(
            36 + k,
            lambda g: xu[3 + k, pl.ds(8 * g, 8)].astype(jnp.int32),
            xu[jnp.minimum(k, 2)],
            not_last_x,
        )
        return carry

    lax.fori_loop(0, 4, low_plane, 0)
    lax.fori_loop(0, 4, high_plane, 0)

    first = iota((RW, 128), 1) % 8 < 4
    wide[...] = jnp.zeros((128, 128), F32)
    lane = iota((8, 128), 1)
    lane_on = jnp.where(
        lane < 8, not_first_y, jnp.where(lane >= 72, not_last_y, 1.0)
    )
    low_on = jnp.where(sub8 < 4, not_first_z, 1.0) * lane_on
    high_on = jnp.where(sub8 < 4, 1.0, not_last_z) * lane_on

    def turned(arr):
        wide[pl.ds(0, RW)] = arr
        return wide[...].T

    for g in range(3):
        count = 16 if g < 2 else 8
        base = 16 * g
        parts = (
            (0, low_on, turned(jnp.where(first, zd[g], zu_own[g])),
             turned(jnp.where(first, zu_own[g], zd[g]))),
            (8, high_on, turned(jnp.where(first, zd_own[g], zu[g])),
             turned(jnp.where(first, zu[g], zd_own[g]))),
        )
        for off, on, labs, bs in parts:
            for k in range(count):
                xp = base + k
                here = on
                if xp < 4:
                    here = on * not_first_x
                if xp >= 36:
                    here = on * not_last_x
                idx = jnp.clip(labs[8 * k : 8 * k + 8].astype(jnp.int32), 0, LABELS - 1)
                vals, centre = entries(idx, here)
                for c in range(6):
                    qsig[c][xp, pl.ds(off, 8)] = vals[c]
                qinv[xp, pl.ds(off, 8)] = centre
                qv0[xp, pl.ds(off, 8)] = pltpu.roll(bs[8 * k : 8 * k + 8], 4, 0)

    def set_patch(patch, rows):
        patch[...] = rows[...].T[:RW]

    lane_main = iota((RW, 128), 1)

    def z_sides(value, patch, xp, at=None):
        p = patch[...] if at is None else patch[at]
        p = pltpu.roll(p, 127 - 2 * xp, 1)
        ln = iota(value.shape, 1)
        left = jnp.where(ln == 0, p, pltpu.roll(value, 1, 1))
        right = jnp.where(ln == 127, p, pltpu.roll(value, 127, 1))
        return left, right

    row_v[...] = jnp.zeros((128, 128), F32)
    row_q[...] = jnp.zeros((128, 128), F32)

    def q_diag(xp, carry):
        c = qinv[xp]
        f1 = q1[xp]
        f2 = q2[xp]
        total = c + (q0[xp + 1] + q0[xp - 1])
        total = total + (pltpu.roll(f1, 1, 1) + pltpu.roll(f1, 127, 1))
        total = total + (pltpu.roll(f2, 1, 0) + pltpu.roll(f2, 15, 0))
        r = jnp.where(c > 0, 1.0 / jnp.where(c > 0, total, 1.0), 0.0)
        qinv[xp] = r
        qmid[xp] = theta * total
        w = qv0[xp] * r
        qv0[xp] = w
        row_q[pl.ds(2 * xp + 1, 1)] = f2[3:4]
        row_q[pl.ds(2 * xp, 1)] = f2[12:13]
        row_v[pl.ds(2 * xp + 1, 1)] = w[3:4]
        row_v[pl.ds(2 * xp, 1)] = w[12:13]
        return carry

    lax.fori_loop(1, XP - 1, q_diag, 0)
    set_patch(patch_q, row_q)
    set_patch(patch_v, row_v)

    def diag_rows(xp, at, size):
        c = inv[xp, pl.ds(at, size)]
        left, right = z_sides(s2[xp, pl.ds(at, size)], patch_q, xp, pl.ds(at, size))
        total = c + (s0[xp + 1, pl.ds(at, size)] + s0[xp - 1, pl.ds(at, size)])
        total = total + (s1[xp, pl.ds(at + 1, size)] + s1[xp, pl.ds(at - 1, size)])
        total = total + (left + right)
        r = jnp.where(c > 0, 1.0 / jnp.where(c > 0, total, 1.0), 0.0)
        rhs = v0[xp, pl.ds(at, size)]
        return r, rhs, rhs * r, theta * total

    def add(acc, value):
        total, lost = acc
        value = value - lost
        new = total + value
        return new, (new - total) - value

    def fold(value):
        return jnp.sum(value.reshape(-1, 8, 128), axis=0)

    def main_diag(xp, acc):
        r8, _, w8, m8 = diag_rows(xp, 71, 8)
        r1, _, w1_, m1 = diag_rows(xp, 1, 8)
        r, rhs, w, m = diag_rows(xp, 8, NY)
        mid[xp, pl.ds(71, 8)] = m8
        mid[xp, pl.ds(1, 8)] = m1
        mid[xp, OWN] = m
        inv[xp, pl.ds(71, 8)] = r8
        inv[xp, pl.ds(1, 8)] = r1
        inv[xp, OWN] = r
        v0[xp, pl.ds(71, 8)] = w8
        v0[xp, pl.ds(1, 8)] = w1_
        v0[xp, OWN] = w
        mine = jnp.logical_and(xp >= 4, xp < 36).astype(F32)
        return add(acc, fold(rhs * w) * mine)

    zero8 = jnp.zeros((8, 128), F32)
    none = (zero8, zero8)
    nu0 = lax.fori_loop(1, XP - 1, main_diag, none)

    def apply(v, w, qv, qw, lo, hi, last):
        def q_first(xp, carry):
            x = qv[xp]
            left = pltpu.roll(x, 1, 0)
            right = pltpu.roll(x, 15, 0)
            qdz[xp] = right - left
            qac[xp] = q2[xp] * (left + right)
            p3[xp] = q3[xp] * x
            p4[xp] = q4[xp] * x
            p5[xp] = q5[xp] * x
            return carry

        lax.fori_loop(lo - 1, hi + 1, q_first, 0)

        def q_second(xp, carry):
            def dy(x):
                return pltpu.roll(x, 127, 1) - pltpu.roll(x, 1, 1)

            x = qv[xp]
            u2 = q2[xp] * x
            q = (p4[xp + 1] - p4[xp - 1]) + dy(p5[xp])
            plus = u2 + q
            minus = u2 - q
            row_q[pl.ds(2 * xp + 1, 1)] = minus[3:4]
            row_q[pl.ds(2 * xp, 1)] = plus[12:13]
            if not last:
                f0 = q0[xp]
                xa, xb = qv[xp + 1], qv[xp - 1]
                r = (qac[xp] - qmid[xp] * x) + (f0 + q0[xp + 1]) * xa + (f0 + q0[xp - 1]) * xb
                u1 = q1[xp] * x
                t = p3[xp + 1] - p3[xp - 1]
                r = r + q1[xp] * (pltpu.roll(x, 127, 1) + pltpu.roll(x, 1, 1))
                r = r + pltpu.roll(u1 + t, 127, 1) + pltpu.roll(u1 - t, 1, 1)
                r = r + q3[xp] * dy(xa - xb)
                r = r + q4[xp] * (qdz[xp + 1] - qdz[xp - 1])
                r = r + q5[xp] * dy(qdz[xp])
                r = r + pltpu.roll(plus, 15, 0) + pltpu.roll(minus, 1, 0)
                out = r * qinv[xp]
                qw[xp] = out
                row_v[pl.ds(2 * xp + 1, 1)] = out[3:4]
                row_v[pl.ds(2 * xp, 1)] = out[12:13]
            return carry

        lax.fori_loop(lo, hi, q_second, 0)
        set_patch(patch_q, row_q)

        def first_pass(xp, carry):
            x = v[xp]
            left, right = z_sides(x, patch_v, xp)
            dz[xp] = right - left
            ac[xp] = s2[xp] * (left + right)
            u3[xp] = s3[xp] * x
            u4[xp] = s4[xp] * x
            u5[xp] = s5[xp] * x
            return carry

        lax.fori_loop(lo - 1, hi + 1, first_pass, 0)

        def rows_of(xp, at, size):
            here = pl.ds(at, size)
            nxt = pl.ds(at + 1, size)
            prv = pl.ds(at - 1, size)
            f0 = s0[xp, here]
            x = v[xp, here]
            r = ac[xp, here] - mid[xp, here] * x
            r = r + (f0 + s0[xp + 1, here]) * v[xp + 1, here]
            r = r + (f0 + s0[xp - 1, here]) * v[xp - 1, here]
            f1 = s1[xp, here]
            r = r + (f1 + s1[xp, nxt]) * v[xp, nxt]
            r = r + (f1 + s1[xp, prv]) * v[xp, prv]
            cross = (v[xp + 1, nxt] - v[xp - 1, nxt]) - (v[xp + 1, prv] - v[xp - 1, prv])
            r = r + s3[xp, here] * cross
            r = r + ((u3[xp + 1, nxt] - u3[xp - 1, nxt]) - (u3[xp + 1, prv] - u3[xp - 1, prv]))
            r = r + s4[xp, here] * (dz[xp + 1, here] - dz[xp - 1, here])
            r = r + s5[xp, here] * (dz[xp, nxt] - dz[xp, prv])
            u2 = s2[xp, here] * x
            q = (u4[xp + 1, here] - u4[xp - 1, here]) + (u5[xp, nxt] - u5[xp, prv])
            p = pltpu.roll(patch_q[here], 127 - 2 * xp, 1)
            ln = iota(q.shape, 1)
            r = r + jnp.where(ln == 127, p, pltpu.roll(u2 + q, 127, 1))
            r = r + jnp.where(ln == 0, p, pltpu.roll(u2 - q, 1, 1))
            return x, r

        def second_pass(xp, acc):
            if last:
                x, r = rows_of(xp, 8, NY)
                return (add(acc[0], fold(x * r)), acc[1])
            for at in (71, 1):
                _, r = rows_of(xp, at, 8)
                w[xp, pl.ds(at, 8)] = r * inv[xp, pl.ds(at, 8)]
            x, r = rows_of(xp, 8, NY)
            out = r * inv[xp, OWN]
            w[xp, OWN] = out
            mine = jnp.logical_and(xp >= 4, xp < 36).astype(F32)
            return add(acc[0], fold(x * r) * mine), add(acc[1], fold(out * r) * mine)

        out = lax.fori_loop(lo, hi, second_pass, (none, none))
        if not last:
            set_patch(patch_v, row_v)
        return out

    nu1, nu2 = apply(v0, v1, qv0, qv1, 2, XP - 2, False)
    nu3, nu4 = apply(v1, v2, qv1, qv2, 3, XP - 3, False)
    nu5, _ = apply(v2, None, qv2, None, 4, XP - 4, True)

    def store(x, carry):
        w0o[x] = v0[x + 4, OWN]
        w1o[x] = v1[x + 4, OWN]
        w2o[x] = v2[x + 4, OWN]
        return carry

    lax.fori_loop(0, NX, store, 0)
    line = jnp.zeros((1, 128), F32)
    at = iota((1, 128), 1)
    line = jnp.where(at == 6, theta, line)
    for k, (nu, _) in enumerate((nu0, nu1, nu2, nu3, nu4, nu5)):
        part = jnp.sum(jnp.sum(nu, axis=0, keepdims=True), axis=1, keepdims=True)
        line = jnp.where(at == k, part, line)
    mom[...] = jnp.broadcast_to(line, mom.shape)


def combine(mom, w0, w1, w2, out):
    total = jnp.sum(mom[...], axis=0, keepdims=True)
    at = iota((1, 128), 1)
    m = [jnp.sum(jnp.where(at == k, total, 0.0), axis=1, keepdims=True) for k in range(7)]
    rest = 1.0 - m[6] * (1.0 / mom.shape[0])
    a = [rest * m[k] - m[k + 1] for k in range(5)]
    tiny = 1e-7

    def ratio(p, q, limit):
        ok = q > limit
        return jnp.where(ok, p / jnp.where(ok, q, 1.0), 0.0)

    l10 = a[1] / a[0]
    l20 = a[2] / a[0]
    d1 = a[2] - l10 * a[1]
    e12 = a[3] - l10 * a[2]
    g1 = m[1] - l10 * m[0]
    l21 = ratio(e12, d1, tiny * a[2])
    d2 = a[4] - l20 * a[2] - l21 * e12
    g2 = m[2] - l20 * m[0] - l21 * g1
    c2 = ratio(g2, d2, tiny * a[4])
    c1 = ratio(g1, d1, tiny * a[2]) - l21 * c2
    c0 = (m[0] - a[1] * c1 - a[2] * c2) / a[0]

    def plane(x, carry):
        out[x] = c0 * w0[x] + c1 * w1[x] + c2 * w2[x]
        return carry

    lax.fori_loop(0, NX, plane, 0)


def vmem():
    return pl.BlockSpec(memory_space=pltpu.VMEM)


def local(labels, conductivity, right_side):
    xu_own = jnp.concatenate([right_side[:3], labels[:4].astype(F32)], 0)
    xl_own = jnp.concatenate([right_side[NX - 3 :], labels[NX - 4 :].astype(F32)], 0)
    xu = ring(xu_own, "gx", -1)
    xl = ring(xl_own, "gx", 1)

    def ends(planes):
        return [
            pl.BlockSpec((planes, 8, 128), lambda i: (0, 0, 0)),
            pl.BlockSpec((planes, 8, 128), lambda i: (0, 7, 0)),
        ]

    packet = jax.ShapeDtypeStruct((XP, 8, 128), F32)
    whole = pl.BlockSpec((XP, 8, 128), lambda i: (0, 0, 0))
    yu_own, yd_own = pl.pallas_call(
        pack_rows,
        grid=(1,),
        in_specs=ends(NX) + ends(NX) + ends(7) + ends(7),
        out_specs=[whole, whole],
        out_shape=[packet, packet],
        name="pack_rows",
    )(labels, labels, right_side, right_side, xu, xu, xl, xl)
    yu = ring(yu_own, "gy", -1)
    yd = ring(yd_own, "gy", 1)

    packet = jax.ShapeDtypeStruct((3, RW, 128), F32)
    zu_own, zd_own = pl.pallas_call(
        pack_lanes,
        in_specs=[vmem()] * 6,
        out_specs=[vmem()] * 2,
        out_shape=[packet, packet],
        scratch_shapes=[pltpu.VMEM((3, RW, 128), F32)] * 2,
        name="pack_lanes",
    )(labels, right_side, xu, xl, yu, yd)
    zu = ring(zu_own, "gz", -1)
    zd = ring(zd_own, "gz", 1)

    block = jax.ShapeDtypeStruct((NX, NY, NZ), F32)
    main = pltpu.VMEM((XP, RW, 128), F32)
    slab = pltpu.VMEM((XP, 16, 128), F32)
    w0, w1, w2, mom = pl.pallas_call(
        sweeps,
        in_specs=[pl.BlockSpec(memory_space=pltpu.SMEM)] + [vmem()] * 10,
        out_specs=[vmem()] * 4,
        out_shape=[block, block, block, jax.ShapeDtypeStruct((128, 128), F32)],
        scratch_shapes=[main] * 16
        + [slab] * 16
        + [pltpu.VMEM((128, 128), F32)]
        + [pltpu.VMEM((RW, 128), F32)] * 2
        + [pltpu.VMEM((128, 128), F32)] * 2,
        compiler_params=pltpu.CompilerParams(vmem_limit_bytes=48 * 1024 * 1024),
        name="sweeps",
    )(conductivity, labels, right_side, xu, xl, yu, yd, zu_own, zd_own, zu, zd)
    mom = lax.all_to_all(mom, ALL, 0, 0, tiled=True)
    return pl.pallas_call(
        combine,
        in_specs=[vmem()] * 4,
        out_specs=vmem(),
        out_shape=block,
        name="combine",
    )(mom, w0, w1, w2)


def solution(mesh):
    spec = P("gx", "gy", "gz")
    return jax.shard_map(
        local, mesh=mesh, in_specs=(spec, P(), spec), out_specs=spec, check_vma=False
    )
```

```python
import jax
import jax.numpy as jnp
from jax import lax
from jax.experimental import pallas as pl
from jax.experimental.pallas import tpu as pltpu
from jax.sharding import PartitionSpec as P

LABELS = 8
ALL = ("gx", "gy", "gz")
NX, NY, NZ = 32, 64, 128
XP, RW = NX + 8, NY + 24
OWN = slice(8, 8 + NY)
F32 = jnp.float32


def ring(arr, axis, step):
    count = lax.axis_size(axis)
    return lax.ppermute(arr, axis, [(i, (i + step) % count) for i in range(count)])


def iota(shape, dim):
    return lax.broadcasted_iota(jnp.int32, shape, dim)


def pack_rows(lab, b, xu, xl, up, down):
    low = iota((8, 128), 0) < 4
    head, tail = pl.ds(0, 8), pl.ds(NY - 8, 8)

    def put(xp, lab_first, lab_last, b_first, b_last):
        up[xp] = jnp.where(low, b_first, pltpu.roll(lab_first, 4, 0))
        down[xp] = jnp.where(low, pltpu.roll(lab_last, 4, 0), b_last)

    for x in range(NX):
        put(x + 4, lab[x, head].astype(F32), lab[x, tail].astype(F32), b[x, head], b[x, tail])
    zero = jnp.zeros((8, 128), F32)
    for k in range(4):
        bk = (xl[k - 1, head], xl[k - 1, tail]) if k else (zero, zero)
        put(k, xl[3 + k, head], xl[3 + k, tail], *bk)
        bk = (xu[k, head], xu[k, tail]) if k < 3 else (zero, zero)
        put(36 + k, xu[3 + k, head], xu[3 + k, tail], *bk)


def rows_lab(yu, yd, xp):
    low = iota((8, 128), 0) < 4
    return pltpu.roll(jnp.where(low, yd[xp], yu[xp]), 4, 0)


def rows_b(yu, yd, xp):
    low = iota((8, 128), 0) < 4
    return jnp.where(low, yu[xp], yd[xp])


def pack_lanes(lab, b, xu, xl, yu, yd, up, down):
    lane = iota((8, 128), 1)
    first = lane % 8 < 4
    zero = jnp.zeros((8, 128), F32)

    def pack(at, lab_of, b_of):
        for g in range(3):
            acc_lab, acc_b = zero, zero
            for k in range(16 if g < 2 else 8):
                hit = lane // 8 == k
                shift = (8 * k + 4) % 128
                turn = lambda t: pltpu.roll(t, shift, 1) if shift else t
                acc_lab = jnp.where(hit, turn(lab_of(16 * g + k)), acc_lab)
                acc_b = jnp.where(hit, turn(b_of(16 * g + k)), acc_b)
            for off in at:
                down[g, off] = jnp.where(first, acc_lab, pltpu.roll(acc_b, 4, 1))
                up[g, off] = jnp.where(first, pltpu.roll(acc_b, 124, 1), acc_lab)

    def rows(rg, carry):
        at = pl.ds(pl.multiple_of(8 * rg, 8), 8)

        def lab_of(xp):
            if xp < 4:
                return xl[3 + xp, at]
            if xp >= 36:
                return xu[xp - 33, at]
            return lab[xp - 4, at].astype(F32)

        def b_of(xp):
            if xp < 4:
                return xl[xp - 1, at] if xp else zero
            if xp >= 36:
                return xu[xp - 36, at] if xp < 39 else zero
            return b[xp - 4, at]

        pack((pl.ds(pl.multiple_of(8 * rg + 8, 8), 8),), lab_of, b_of)
        return carry

    lax.fori_loop(0, 8, rows, 0)
    pack(
        (pl.ds(0, 8), pl.ds(72, 8)),
        lambda xp: rows_lab(yu, yd, xp),
        lambda xp: rows_b(yu, yd, xp),
    )


def group(g):
    return pl.ds(8 + 8 * g, 8)


def sweeps(
    cond, lab, b, xu, xl, yu, yd, zu_own, zd_own, zu, zd,
    w0o, w1o, w2o, mom,
    f0, f1, f2, f2l, s3, s4, s5, inv, mid, v0, v1, v2, dz, ac, u3, u4, u5,
    q0, q1, q2, q3, q4, q5, qinv, qmid, qv0, qv1, qv2, qdz, qac, p3, p4, p5,
    wide, patch_v, patch_q, row_v, row_q,
):
    s0, s1, s2 = u3, u4, dz
    sig = (s0, s1, s2, s3, s4, s5)
    qsig = (q0, q1, q2, q3, q4, q5)
    gx, gy, gz = (lax.axis_index(a) for a in ALL)
    not_first_x = (gx > 0).astype(F32)
    not_last_x = (gx < lax.axis_size("gx") - 1).astype(F32)
    not_first_y = (gy > 0).astype(F32)
    not_last_y = (gy < lax.axis_size("gy") - 1).astype(F32)
    not_first_z = (gz > 0).astype(F32)
    not_last_z = (gz < lax.axis_size("gz") - 1).astype(F32)

    sub8 = iota((8, 128), 0)
    ln = iota((8, 128), 1)
    tables = []
    for c in range(7):
        t = jnp.zeros((8, 128), F32)
        scale = 0.5 if c < 3 else (0.25 if c < 6 else 1.0)
        for l in range(LABELS):
            t = jnp.where(sub8 == l, cond[c, l] * scale, t)
        tables.append(t)

    mass = sum(cond[6, l] for l in range(LABELS))
    faces = sum(cond[c, l] for c in range(3) for l in range(LABELS)) * 2.0
    theta = jnp.full((1, 128), faces, F32) / jnp.full((1, 128), faces + mass, F32)

    def look(c, idx):
        return jnp.take_along_axis(tables[c], idx, axis=0, mode="promise_in_bounds")

    def entries(idx, on):
        vals = [look(c, idx) for c in range(7)]
        if on is not None:
            vals = [v * on for v in vals]
        centre = vals[6] + 2.0 * (vals[0] + vals[1] + vals[2])
        return vals[:6], centre

    row_on = jnp.where(sub8 < 4, not_last_y, not_first_y)

    def put(ref, xp, g, value):
        ref[xp, group(g)] = value
        if g == 8:
            ref[xp, pl.ds(0, 8)] = value
        if g == 0:
            ref[xp, pl.ds(80, 8)] = value

    def table_plane(xp, labels_of, b_of, on):
        for g in range(9):
            if g < 8:
                vals, centre = entries(labels_of(g), on)
                v0[xp, group(g)] = b_of(g)
            else:
                vals, centre = entries(
                    rows_lab(yu, yd, xp).astype(jnp.int32),
                    row_on if on is None else row_on * on,
                )
                v0[xp, group(g)] = rows_b(yu, yd, xp)
            for c in range(6):
                if c == 1:
                    put(s1, xp, g, vals[1])
                else:
                    sig[c][xp, group(g)] = vals[c]
            inv[xp, group(g)] = centre

    def own_plane(x, carry):
        table_plane(
            x + 4, lambda g: lab[x, pl.ds(8 * g, 8)], lambda g: b[x, pl.ds(8 * g, 8)], None
        )
        return carry

    lax.fori_loop(0, NX, own_plane, 0)

    def low_plane(k, carry):
        table_plane(
            k,
            lambda g: xl[3 + k, pl.ds(8 * g, 8)].astype(jnp.int32),
            lambda g: xl[jnp.maximum(k - 1, 0), pl.ds(8 * g, 8)],
            not_first_x,
        )
        return carry

    def high_plane(k, carry):
        table_plane(
            36 + k,
            lambda g: xu[3 + k, pl.ds(8 * g, 8)].astype(jnp.int32),
            lambda g: xu[jnp.minimum(k, 2), pl.ds(8 * g, 8)],
            not_last_x,
        )
        return carry

    lax.fori_loop(0, 4, low_plane, 0)
    lax.fori_loop(0, 4, high_plane, 0)

    first = iota((80, 128), 1) % 8 < 4
    wide[...] = jnp.zeros((128, 128), F32)
    lane_on = jnp.where(ln < 8, not_first_y, jnp.where(ln >= 72, not_last_y, 1.0))
    low_on = jnp.where(sub8 < 4, not_first_z, 1.0) * lane_on
    high_on = jnp.where(sub8 < 4, 1.0, not_last_z) * lane_on

    def turned(arr):
        wide[pl.ds(0, 80)] = arr
        return wide[...].T

    for g in range(3):
        count = 16 if g < 2 else 8
        parts = (
            (0, low_on, turned(jnp.where(first, zd[g], zu_own[g])),
             turned(jnp.where(first, zu_own[g], zd[g]))),
            (8, high_on, turned(jnp.where(first, zd_own[g], zu[g])),
             turned(jnp.where(first, zu[g], zd_own[g]))),
        )
        for off, on, labs, bs in parts:
            for k in range(count):
                xp = 16 * g + k
                here = on
                if xp < 4:
                    here = on * not_first_x
                if xp >= 36:
                    here = on * not_last_x
                idx = jnp.clip(labs[8 * k : 8 * k + 8].astype(jnp.int32), 0, LABELS - 1)
                vals, centre = entries(idx, here)
                for c in range(6):
                    qsig[c][xp + 1, pl.ds(off, 8)] = vals[c]
                qinv[xp + 1, pl.ds(off, 8)] = centre
                qv0[xp + 1, pl.ds(off, 8)] = pltpu.roll(bs[8 * k : 8 * k + 8], 4, 0)

    def set_rows(ref, xp, values):
        for k in range(values.shape[0]):
            ref[pl.ds(2 * (xp + k) + 1, 1)] = values[k, 3:4]
            ref[pl.ds(2 * (xp + k), 1)] = values[k, 12:13]

    def set_patch(patch, rows):
        t = rows[...].T
        patch[...] = t[:80]
        patch[pl.ds(72, 8)] = jnp.where(sub8 < 4, t[72:80], t[:8])

    def sides(value, patch, xp, g):
        p = pltpu.roll(patch[group(g)], 127 - 2 * xp, 1)
        left = jnp.where(ln == 0, p, pltpu.roll(value, 1, 1))
        right = jnp.where(ln == 127, p, pltpu.roll(value, 127, 1))
        return left, right

    QB = 8

    def q_loop(body):
        lax.fori_loop(0, XP // QB, lambda i, c: body(QB * i) or c, 0)

    def lanes(x, step):
        return pltpu.roll(x, step % 128, 2)

    def subs(x, step):
        return pltpu.roll(x, step % 16, 1)

    row_v[...] = jnp.zeros((128, 128), F32)
    row_q[...] = jnp.zeros((128, 128), F32)

    def reciprocal(centre, total):
        return jnp.where(centre > 0, 1.0 / jnp.where(centre > 0, total, 1.0), 0.0)

    def q_diag(xp):
        at = pl.ds(xp + 1, QB)
        c = qinv[at]
        b1 = q1[at]
        b2 = q2[at]
        total = c + (q0[pl.ds(xp + 2, QB)] + q0[pl.ds(xp, QB)])
        total = total + (lanes(b1, 1) + lanes(b1, -1))
        total = total + (subs(b2, 1) + subs(b2, -1))
        r = reciprocal(c, total)
        qinv[at] = r
        qmid[at] = theta * total
        w = qv0[at] * r
        qv0[at] = w
        set_rows(row_q, xp, b2)
        set_rows(row_v, xp, w)

    q_loop(q_diag)
    set_patch(patch_q, row_q)
    set_patch(patch_v, row_v)

    def add(acc, value):
        total, lost = acc
        value = value - lost
        new = total + value
        return new, (new - total) - value

    def tree(values):
        while len(values) > 1:
            values = [sum(values[i : i + 2]) for i in range(0, len(values), 2)]
        return values[0]

    zero8 = jnp.zeros((8, 128), F32)
    none = (zero8, zero8)

    def blocks(body, extra, sums):
        if extra:
            lax.fori_loop(
                0, 2, lambda i, c: body(4 - extra + (32 + extra) * i, extra, None) or c, 0
            )
        return lax.fori_loop(0, NX // 4, lambda i, acc: body(4 * i + 4, 4, acc), sums)

    def diag_block(xp0, n, acc):
        for g in range(9):
            at, nxt, prv = group(g), pl.ds(9 + 8 * g, 8), pl.ds(7 + 8 * g, 8)
            faces_x = [s0[xp0 - 1 + i, at] for i in range(n + 2)]
            parts = []
            for i in range(n):
                xp = xp0 + i
                c = inv[xp, at]
                a1, a1n = s1[xp, at], s1[xp, nxt]
                a2 = s2[xp, at]
                left, right = sides(a2, patch_q, xp, g)
                total = c + (faces_x[i + 2] + faces_x[i])
                total = total + (a1n + s1[xp, prv])
                total = total + (left + right)
                r = reciprocal(c, total)
                rhs = v0[xp, at]
                w = rhs * r
                inv[xp, at] = r
                mid[xp, at] = theta * total
                put(v0, xp, g, w)
                f0[xp, at] = faces_x[i + 1] + faces_x[i + 2]
                put(f1, xp, g, a1 + a1n)
                f2[xp, at] = a2 + right
                f2l[xp, at] = a2 + left
                parts.append(rhs * w)
            if acc is not None and g < 8:
                acc = add(acc, tree(parts))
        return acc

    nu0 = blocks(diag_block, 3, none)

    def apply(v, w, qv, qw, extra, last):
        def q_first(xp):
            at = pl.ds(xp + 1, QB)
            x = qv[at]
            left = subs(x, 1)
            right = subs(x, -1)
            qdz[at] = right - left
            qac[at] = q2[at] * (left + right)
            p3[at] = q3[at] * x
            p4[at] = q4[at] * x
            p5[at] = q5[at] * x

        q_loop(q_first)

        def q_second(xp):
            at, nx, pr = pl.ds(xp + 1, QB), pl.ds(xp + 2, QB), pl.ds(xp, QB)

            def dy(x):
                return lanes(x, -1) - lanes(x, 1)

            q = (p4[nx] - p4[pr]) + dy(p5[at])
            set_rows(row_q, xp, q)
            if not last:
                x = qv[at]
                u2 = q2[at] * x
                b0 = q0[at]
                xa, xb = qv[nx], qv[pr]
                r = (qac[at] - qmid[at] * x) + (b0 + q0[nx]) * xa + (b0 + q0[pr]) * xb
                u1 = q1[at] * x
                t = p3[nx] - p3[pr]
                r = r + q1[at] * (lanes(x, -1) + lanes(x, 1))
                r = r + lanes(u1 + t, -1) + lanes(u1 - t, 1)
                r = r + q3[at] * dy(xa - xb)
                r = r + q4[at] * (qdz[nx] - qdz[pr])
                r = r + q5[at] * dy(qdz[at])
                r = r + subs(u2 + q, -1) + subs(u2 - q, 1)
                out = r * qinv[at]
                qw[at] = out
                set_rows(row_v, xp, out)

        q_loop(q_second)
        set_patch(patch_q, row_q)

        def first_block(xp0, n, acc):
            for g in range(9):
                at = group(g)
                for xp in [xp0 + i for i in range(n)]:
                    x = v[xp, at]
                    left, right = sides(x, patch_v, xp, g)
                    put(dz, xp, g, right - left)
                    ac[xp, at] = f2[xp, at] * right + f2l[xp, at] * left
                    put(u3, xp, g, s3[xp, at] * x)
                    u4[xp, at] = s4[xp, at] * x
                    put(u5, xp, g, s5[xp, at] * x)
            return acc

        blocks(first_block, extra + 1, 0)

        def second_block(xp0, n, acc):
            def start(g):
                at, nxt, prv = group(g), pl.ds(9 + 8 * g, 8), pl.ds(7 + 8 * g, 8)
                a4 = [u4[xp0 - 1 + i, at] for i in range(n + 2)]
                out = []
                for i in range(n):
                    xp = xp0 + i
                    q = (a4[i + 2] - a4[i]) + (u5[xp, nxt] - u5[xp, prv])
                    left, right = sides(q, patch_q, xp, g)
                    out.append(right - left)
                return out

            def finish(g, qs, acc):
                at, nxt, prv = group(g), pl.ds(9 + 8 * g, 8), pl.ds(7 + 8 * g, 8)
                vh = [v[xp0 - 1 + i, at] for i in range(n + 2)]
                vn = [v[xp0 - 1 + i, nxt] for i in range(n + 2)]
                vp = [v[xp0 - 1 + i, prv] for i in range(n + 2)]
                un = [u3[xp0 - 1 + i, nxt] for i in range(n + 2)]
                up = [u3[xp0 - 1 + i, prv] for i in range(n + 2)]
                zh = [dz[xp0 - 1 + i, at] for i in range(n + 2)]
                fx = [f0[xp0 - 1 + i, at] for i in range(n + 1)]
                dots, norms = [], []
                for i in range(n):
                    xp = xp0 + i
                    x = vh[i + 1]
                    r = ac[xp, at] - mid[xp, at] * x
                    r = r + (fx[i + 1] * vh[i + 2] + fx[i] * vh[i])
                    r = r + (f1[xp, at] * vn[i + 1] + f1[xp, prv] * vp[i + 1])
                    r = r + s3[xp, at] * ((vn[i + 2] - vn[i]) - (vp[i + 2] - vp[i]))
                    r = r + ((un[i + 2] - un[i]) - (up[i + 2] - up[i]))
                    r = r + s4[xp, at] * (zh[i + 2] - zh[i])
                    r = r + s5[xp, at] * (dz[xp, nxt] - dz[xp, prv])
                    r = r + qs[i]
                    dots.append(x * r)
                    if not last:
                        out = r * inv[xp, at]
                        put(w, xp, g, out)
                        norms.append(out * r)
                if acc is None or g == 8:
                    return acc
                if last:
                    return add(acc[0], tree(dots)), acc[1]
                return add(acc[0], tree(dots)), add(acc[1], tree(norms))

            count = 8 if last else 9
            ahead = 2
            pending = [start(g) for g in range(ahead)]
            for g in range(count):
                if g + ahead < count:
                    pending.append(start(g + ahead))
                acc = finish(g, pending.pop(0), acc)
            return acc

        out = blocks(second_block, extra, (none, none))
        if not last:
            set_patch(patch_v, row_v)
        return out

    nu1, nu2 = apply(v0, v1, qv0, qv1, 2, False)
    nu3, nu4 = apply(v1, v2, qv1, qv2, 1, False)
    nu5, _ = apply(v2, None, qv2, None, 0, True)

    def store(x, carry):
        w0o[x] = v0[x + 4, OWN]
        w1o[x] = v1[x + 4, OWN]
        w2o[x] = v2[x + 4, OWN]
        return carry

    lax.fori_loop(0, NX, store, 0)
    line = jnp.zeros((1, 128), F32)
    at = iota((1, 128), 1)
    line = jnp.where(at == 6, theta, line)
    for k, (nu, _) in enumerate((nu0, nu1, nu2, nu3, nu4, nu5)):
        part = jnp.sum(jnp.sum(nu, axis=0, keepdims=True), axis=1, keepdims=True)
        line = jnp.where(at == k, part, line)
    mom[...] = jnp.broadcast_to(line, mom.shape)


def combine(mom, w0, w1, w2, out):
    total = jnp.sum(mom[...], axis=0, keepdims=True)
    at = iota((1, 128), 1)
    m = [jnp.sum(jnp.where(at == k, total, 0.0), axis=1, keepdims=True) for k in range(7)]
    rest = 1.0 - m[6] * (1.0 / mom.shape[0])
    a = [rest * m[k] - m[k + 1] for k in range(5)]
    tiny = 1e-7

    def ratio(p, q, limit):
        ok = q > limit
        return jnp.where(ok, p / jnp.where(ok, q, 1.0), 0.0)

    l10 = a[1] / a[0]
    l20 = a[2] / a[0]
    d1 = a[2] - l10 * a[1]
    e12 = a[3] - l10 * a[2]
    g1 = m[1] - l10 * m[0]
    l21 = ratio(e12, d1, tiny * a[2])
    d2 = a[4] - l20 * a[2] - l21 * e12
    g2 = m[2] - l20 * m[0] - l21 * g1
    c2 = ratio(g2, d2, tiny * a[4])
    c1 = ratio(g1, d1, tiny * a[2]) - l21 * c2
    c0 = (m[0] - a[1] * c1 - a[2] * c2) / a[0]

    def plane(x, carry):
        out[x] = c0 * w0[x] + c1 * w1[x] + c2 * w2[x]
        return carry

    lax.fori_loop(0, NX, plane, 0)


def vmem():
    return pl.BlockSpec(memory_space=pltpu.VMEM)


def local(labels, conductivity, right_side):
    xu_own = jnp.concatenate([right_side[:3], labels[:4].astype(F32)], 0)
    xl_own = jnp.concatenate([right_side[NX - 3 :], labels[NX - 4 :].astype(F32)], 0)
    xu = ring(xu_own, "gx", -1)
    xl = ring(xl_own, "gx", 1)

    packet = jax.ShapeDtypeStruct((XP, 8, 128), F32)
    yu_own, yd_own = call(pack_rows, 4, [packet] * 2, 4)(labels, right_side, xu, xl)
    yu = ring(yu_own, "gy", -1)
    yd = ring(yd_own, "gy", 1)

    packet = jax.ShapeDtypeStruct((3, 80, 128), F32)
    zu_own, zd_own = call(pack_lanes, 6, [packet] * 2, 6)(labels, right_side, xu, xl, yu, yd)
    zu = ring(zu_own, "gz", -1)
    zd = ring(zd_own, "gz", 1)

    block = jax.ShapeDtypeStruct((NX, NY, NZ), F32)
    square = pltpu.VMEM((128, 128), F32)
    patch = pltpu.VMEM((80, 128), F32)
    w0, w1, w2, mom = pl.pallas_call(
        sweeps,
        in_specs=[pl.BlockSpec(memory_space=pltpu.SMEM)] + [vmem()] * 10,
        out_specs=[vmem()] * 4,
        out_shape=[block, block, block, jax.ShapeDtypeStruct((128, 128), F32)],
        scratch_shapes=[pltpu.VMEM((XP, RW, 128), F32)] * 17
        + [pltpu.VMEM((XP + 2, 16, 128), F32)] * 16
        + [square, patch, patch, square, square],
        compiler_params=pltpu.CompilerParams(vmem_limit_bytes=48 * 2**20),
        name="sweeps",
    )(conductivity, labels, right_side, xu, xl, yu, yd, zu_own, zd_own, zu, zd)
    mom = lax.all_to_all(mom, ALL, 0, 0, tiled=True)
    return call(combine, 4, block, 6)(mom, w0, w1, w2)


def call(kernel, inputs, shapes, mib):
    many = isinstance(shapes, list)
    return pl.pallas_call(
        kernel,
        in_specs=[vmem()] * inputs,
        out_specs=[vmem()] * len(shapes) if many else vmem(),
        out_shape=shapes,
        compiler_params=pltpu.CompilerParams(vmem_limit_bytes=mib * 2**20),
        name=kernel.__name__,
    )


def solution(mesh):
    spec = P("gx", "gy", "gz")
    return jax.shard_map(
        local, mesh=mesh, in_specs=(spec, P(), spec), out_specs=spec, check_vma=False
    )
```

```python
import jax
import jax.numpy as jnp
from jax import lax
from jax.experimental import pallas as pl
from jax.experimental.pallas import tpu as pltpu
from jax.sharding import PartitionSpec as P

LABELS = 8
ALL = ("gx", "gy", "gz")
NX, NY, NZ = 32, 64, 128
XP, RW = NX + 10, NY + 24
OWN = slice(8, 8 + NY)
F32 = jnp.float32


def ring(arr, axis, step):
    count = lax.axis_size(axis)
    return lax.ppermute(arr, axis, [(i, (i + step) % count) for i in range(count)])


def iota(shape, dim):
    return lax.broadcasted_iota(jnp.int32, shape, dim)


def pack_rows(lab0, lab7, b0, b7, xu, xl, up, down):
    low = iota((8, 128), 0) < 4
    head, tail = pl.ds(0, 8), pl.ds(NY - 8, 8)

    def put(xp, lab_first, lab_last, b_first, b_last):
        up[xp] = jnp.where(low, b_first, pltpu.roll(lab_first, 4, 0))
        down[xp] = jnp.where(low, pltpu.roll(lab_last, 4, 0), b_last)

    for x in range(NX):
        put(x + 4, lab0[x].astype(F32), lab7[x].astype(F32), b0[x], b7[x])
    zero = jnp.zeros((8, 128), F32)
    for k in range(4):
        bk = (xl[k - 1, head], xl[k - 1, tail]) if k else (zero, zero)
        put(k, xl[3 + k, head], xl[3 + k, tail], *bk)
        bk = (xu[k, head], xu[k, tail]) if k < 3 else (zero, zero)
        put(36 + k, xu[3 + k, head], xu[3 + k, tail], *bk)


def rows_lab(yu, yd, xp):
    low = iota((8, 128), 0) < 4
    return pltpu.roll(jnp.where(low, yd[xp], yu[xp]), 4, 0)


def rows_b(yu, yd, xp):
    low = iota((8, 128), 0) < 4
    return jnp.where(low, yu[xp], yd[xp])


def pack_lanes(lab, b, xu, xl, yu, yd, up, down):
    lane = iota((8, 128), 1)
    first = lane % 8 < 4
    zero = jnp.zeros((8, 128), F32)

    def pack(at, lab_of, b_of):
        for g in range(3):
            acc_lab, acc_b = zero, zero
            for k in range(16 if g < 2 else 8):
                hit = lane // 8 == k
                shift = (8 * k + 4) % 128
                turn = lambda t: pltpu.roll(t, shift, 1) if shift else t
                acc_lab = jnp.where(hit, turn(lab_of(16 * g + k)), acc_lab)
                acc_b = jnp.where(hit, turn(b_of(16 * g + k)), acc_b)
            for off in at:
                down[g, off] = jnp.where(first, acc_lab, pltpu.roll(acc_b, 4, 1))
                up[g, off] = jnp.where(first, pltpu.roll(acc_b, 124, 1), acc_lab)

    def rows(rg, carry):
        at = pl.ds(pl.multiple_of(8 * rg, 8), 8)

        def lab_of(xp):
            if xp < 4:
                return xl[3 + xp, at]
            if xp >= 36:
                return xu[xp - 33, at]
            return lab[xp - 4, at].astype(F32)

        def b_of(xp):
            if xp < 4:
                return xl[xp - 1, at] if xp else zero
            if xp >= 36:
                return xu[xp - 36, at] if xp < 39 else zero
            return b[xp - 4, at]

        pack((pl.ds(pl.multiple_of(8 * rg + 8, 8), 8),), lab_of, b_of)
        return carry

    lax.fori_loop(0, 8, rows, 0)
    pack(
        (pl.ds(0, 8), pl.ds(72, 8)),
        lambda xp: rows_lab(yu, yd, xp),
        lambda xp: rows_b(yu, yd, xp),
    )


def group(g):
    return pl.ds(8 + 8 * g, 8)


def sweeps(
    cond, lab, b, xu, xl, yu, yd, zu_own, zd_own, zu, zd,
    w0o, w1o, w2o, mom,
    f0, f1, f2, f2l, s3, s4, s5, inv, mid, v0, v1, v2, dz, ac, u3, u4, u5,
    q0, q1, q2, q3, q4, q5, qf1, qf1l, qf2, qf2l, qinv, qmid, qv0, qv1, qv2,
    qdy, p3, p4, p5,
    wide, patch_q, row_q,
):
    s0, s1, s2 = u3, u4, dz
    sig = (s0, s1, s2, s3, s4, s5)
    qsig = (q0, q1, q2, q3, q4, q5)
    gx, gy, gz = (lax.axis_index(a) for a in ALL)
    not_first_x = (gx > 0).astype(F32)
    not_last_x = (gx < lax.axis_size("gx") - 1).astype(F32)
    not_first_y = (gy > 0).astype(F32)
    not_last_y = (gy < lax.axis_size("gy") - 1).astype(F32)
    not_first_z = (gz > 0).astype(F32)
    not_last_z = (gz < lax.axis_size("gz") - 1).astype(F32)

    sub8 = iota((8, 128), 0)
    ln = iota((8, 128), 1)
    tables = []
    for c in range(7):
        t = jnp.zeros((8, 128), F32)
        scale = 0.5 if c < 3 else (0.25 if c < 6 else 1.0)
        for l in range(LABELS):
            t = jnp.where(sub8 == l, cond[c, l] * scale, t)
        tables.append(t)

    mass = sum(cond[6, l] for l in range(LABELS))
    faces = sum(cond[c, l] for c in range(3) for l in range(LABELS)) * 2.0
    theta = jnp.full((1, 128), faces, F32) / jnp.full((1, 128), faces + mass, F32)

    def look(c, idx):
        return jnp.take_along_axis(tables[c], idx, axis=0, mode="promise_in_bounds")

    def entries(idx, on):
        vals = [look(c, idx) for c in range(7)]
        if on is not None:
            vals = [v * on for v in vals]
        centre = vals[6] + 2.0 * (vals[0] + vals[1] + vals[2])
        return vals[:6], centre

    row_on = jnp.where(sub8 < 4, not_last_y, not_first_y)

    def put(ref, xp, g, value):
        ref[xp, group(g)] = value
        if g == 8:
            ref[xp, pl.ds(0, 8)] = value
        if g == 0:
            ref[xp, pl.ds(80, 8)] = value

    def table_plane(xp, labels_of, b_of, on):
        for g in range(9):
            if g < 8:
                vals, centre = entries(labels_of(g), on)
                v0[xp, group(g)] = b_of(g)
            else:
                vals, centre = entries(
                    rows_lab(yu, yd, xp).astype(jnp.int32),
                    row_on if on is None else row_on * on,
                )
                v0[xp, group(g)] = rows_b(yu, yd, xp)
            for c in range(6):
                if c == 1:
                    put(s1, xp, g, vals[1])
                else:
                    sig[c][xp, group(g)] = vals[c]
            inv[xp, group(g)] = centre

    def own_plane(x, carry):
        table_plane(
            x + 4, lambda g: lab[x, pl.ds(8 * g, 8)], lambda g: b[x, pl.ds(8 * g, 8)], None
        )
        return carry

    lax.fori_loop(0, NX, own_plane, 0)

    def low_plane(k, carry):
        table_plane(
            k,
            lambda g: xl[3 + k, pl.ds(8 * g, 8)].astype(jnp.int32),
            lambda g: xl[jnp.maximum(k - 1, 0), pl.ds(8 * g, 8)],
            not_first_x,
        )
        return carry

    def high_plane(k, carry):
        table_plane(
            36 + k,
            lambda g: xu[3 + k, pl.ds(8 * g, 8)].astype(jnp.int32),
            lambda g: xu[jnp.minimum(k, 2), pl.ds(8 * g, 8)],
            not_last_x,
        )
        return carry

    lax.fori_loop(0, 4, low_plane, 0)
    lax.fori_loop(0, 4, high_plane, 0)

    first = iota((80, 128), 1) % 8 < 4
    wide[...] = jnp.zeros((128, 128), F32)
    lane_on = jnp.where(ln < 8, not_first_y, jnp.where(ln >= 72, not_last_y, 1.0))
    low_on = jnp.where(sub8 < 4, not_first_z, 1.0) * lane_on
    high_on = jnp.where(sub8 < 4, 1.0, not_last_z) * lane_on

    def turned(arr):
        wide[pl.ds(0, 80)] = arr
        return wide[...].T

    for g in range(3):
        count = 16 if g < 2 else 8
        parts = (
            (0, low_on, turned(jnp.where(first, zd[g], zu_own[g])),
             turned(jnp.where(first, zu_own[g], zd[g]))),
            (8, high_on, turned(jnp.where(first, zd_own[g], zu[g])),
             turned(jnp.where(first, zu[g], zd_own[g]))),
        )
        for off, on, labs, bs in parts:
            for k in range(count):
                xp = 16 * g + k
                here = on
                if xp < 4:
                    here = on * not_first_x
                if xp >= 36:
                    here = on * not_last_x
                idx = jnp.clip(labs[8 * k : 8 * k + 8].astype(jnp.int32), 0, LABELS - 1)
                vals, centre = entries(idx, here)
                for c in range(6):
                    qsig[c][xp + 1, pl.ds(off, 8)] = vals[c]
                qinv[xp + 1, pl.ds(off, 8)] = centre
                qv0[xp + 1, pl.ds(off, 8)] = pltpu.roll(bs[8 * k : 8 * k + 8], 4, 0)

    def set_rows(ref, xp, for_first, for_last):
        for k in range(QB):
            ref[pl.ds(2 * (xp + k) + 1, 1)] = for_first[k]
            ref[pl.ds(2 * (xp + k), 1)] = for_last[k]

    def set_patch(patch, rows):
        t = rows[...].T
        patch[...] = t[:80]
        patch[pl.ds(72, 8)] = jnp.where(sub8 < 4, t[72:80], t[:8])

    def sides(value, patch, xp, g):
        p = pltpu.roll(patch[group(g)], 127 - 2 * xp, 1)
        left = jnp.where(ln == 0, p, pltpu.roll(value, 1, 1))
        right = jnp.where(ln == 127, p, pltpu.roll(value, 127, 1))
        return left, right

    QB = 8

    def q_loop(body):
        lax.fori_loop(0, (NX + 8) // QB, lambda i, c: body(QB * i) or c, 0)

    def lanes(x, step):
        return pltpu.roll(x, step % 128, 2)

    def subs(x, step):
        return pltpu.roll(x, step % 16, 1)

    row_q[...] = jnp.zeros((128, 128), F32)

    def reciprocal(centre, total):
        return jnp.where(centre > 0, 1.0 / jnp.where(centre > 0, total, 1.0), 0.0)

    def q_diag(xp):
        at = pl.ds(xp + 1, QB)
        c = qinv[at]
        b1 = q1[at]
        b2 = q2[at]
        r1, l1 = lanes(b1, -1), lanes(b1, 1)
        r2, l2 = subs(b2, -1), subs(b2, 1)
        total = c + (q0[pl.ds(xp + 2, QB)] + q0[pl.ds(xp, QB)])
        total = total + (l1 + r1)
        total = total + (l2 + r2)
        qf1[at] = b1 + r1
        qf1l[at] = b1 + l1
        qf2[at] = b2 + r2
        qf2l[at] = b2 + l2
        r = reciprocal(c, total)
        qinv[at] = r
        qmid[at] = theta * total
        w = qv0[at] * r
        qv0[at] = w
        set_rows(row_q, xp, b2[:, 3:4], b2[:, 12:13])

    q_loop(q_diag)
    set_patch(patch_q, row_q)

    def add(acc, value):
        total, lost = acc
        value = value - lost
        new = total + value
        return new, (new - total) - value

    def tree(values):
        while len(values) > 1:
            values = [sum(values[i : i + 2]) for i in range(0, len(values), 2)]
        return values[0]

    zero8 = jnp.zeros((8, 128), F32)
    none = (zero8, zero8)

    def blocks(body, extra, sums):
        if extra:
            lax.fori_loop(
                0, 2, lambda i, c: body(4 - extra + (32 + extra) * i, extra, None) or c, 0
            )
        return lax.fori_loop(0, NX // 4, lambda i, acc: body(4 * i + 4, 4, acc), sums)

    def diag_block(xp0, n, acc):
        for g in range(9):
            at, nxt, prv = group(g), pl.ds(9 + 8 * g, 8), pl.ds(7 + 8 * g, 8)
            faces_x = [s0[xp0 - 1 + i, at] for i in range(n + 2)]
            parts = []
            for i in range(n):
                xp = xp0 + i
                c = inv[xp, at]
                a1, a1n = s1[xp, at], s1[xp, nxt]
                a2 = s2[xp, at]
                left, right = sides(a2, patch_q, xp, g)
                total = c + (faces_x[i + 2] + faces_x[i])
                total = total + (a1n + s1[xp, prv])
                total = total + (left + right)
                r = reciprocal(c, total)
                rhs = v0[xp, at]
                w = rhs * r
                inv[xp, at] = r
                mid[xp, at] = theta * total
                put(v0, xp, g, w)
                f0[xp, at] = faces_x[i + 1] + faces_x[i + 2]
                put(f1, xp, g, a1 + a1n)
                f2[xp, at] = a2 + right
                f2l[xp, at] = a2 + left
                parts.append(rhs * w)
            if acc is not None and g < 8:
                acc = add(acc, tree(parts))
        return acc

    nu0 = blocks(diag_block, 3, none)

    def apply(v, w, qv, qw, extra, last):
        def q_first(xp):
            at = pl.ds(xp + 1, QB)
            x = qv[at]
            p4[at] = q4[at] * x
            p5[at] = q5[at] * x
            if not last:
                right, left = lanes(x, -1), lanes(x, 1)
                qdy[at] = right - left
                p3[at] = q3[at] * x
                r = qf2[at] * subs(x, -1) + qf2l[at] * subs(x, 1)
                r = r + (qf1[at] * right + qf1l[at] * left)
                qw[at] = r - qmid[at] * x

        q_loop(q_first)

        def q_second(xp):
            at, nx, pr = pl.ds(xp + 1, QB), pl.ds(xp + 2, QB), pl.ds(xp, QB)
            xa, x5 = qv[nx], p5[at]
            if not last:
                xb = qv[pr]
                dx = xa - xb
                dx4 = p4[nx] - p4[pr]
                y = qdy[at]
            x = qv[at]
            if last:
                q = p4[nx] + lanes(x5, -1)
                e, ex, eq = (t[:, :8] - t[:, 8:] for t in (x, xa, q))
                ey = pltpu.roll(e, 127, 2)
            else:
                q = dx4 + (lanes(x5, -1) - lanes(x5, 1))
                e, ex, ey, eq = (t[:, :8] - t[:, 8:] for t in (x, dx, y, q))

            def turn(t, step):
                return pltpu.roll(t, step % 8, 1)

            b4, b5 = q4[at], q5[at]
            first = -(b4[:, :8] * turn(ex, 1) + b5[:, :8] * turn(ey, 1)) - turn(eq, 1)
            if not last:
                first = first + qf2l[at][:, :8] * turn(e, 1)
            final = qf2[at][:, 8:] * turn(e, -1) + b4[:, 8:] * turn(ex, -1)
            final = final + b5[:, 8:] * turn(ey, -1) + turn(eq, -1)
            set_rows(row_q, xp, first[:, 4:5], -final[:, 3:4])
            if not last:
                b0 = q0[at]
                t = (p3[nx] - p3[pr]) + (subs(x5, -1) - subs(x5, 1))
                r = qw[at] + (b0 + q0[nx]) * xa + (b0 + q0[pr]) * xb
                r = r + (lanes(t, -1) - lanes(t, 1))
                r = r + q3[at] * (qdy[nx] - qdy[pr])
                r = r + b4 * (subs(dx, -1) - subs(dx, 1))
                r = r + b5 * (subs(y, -1) - subs(y, 1))
                r = r + (subs(dx4, -1) - subs(dx4, 1))
                qw[at] = r * qinv[at]

        q_loop(q_second)
        set_patch(patch_q, row_q)

        def first(g, xps):
            at = group(g)
            for xp in xps:
                x = v[xp, at]
                left, right = pltpu.roll(x, 1, 1), pltpu.roll(x, 127, 1)
                put(dz, xp, g, right - left)
                if last:
                    ac[xp, at] = f2[xp, at] * right
                else:
                    ac[xp, at] = f2[xp, at] * right + f2l[xp, at] * left
                put(u3, xp, g, s3[xp, at] * x)
                u4[xp, at] = s4[xp, at] * x
                put(u5, xp, g, s5[xp, at] * x)

        def second_block(xp0, n, acc, then=None):
            def start(g):
                at, nxt, prv = group(g), pl.ds(9 + 8 * g, 8), pl.ds(7 + 8 * g, 8)
                a4 = [u4[xp0 - 1 + i, at] for i in range(n + 2)]
                out = []
                for i in range(n):
                    xp = xp0 + i
                    if last:
                        q = a4[i + 2] + u5[xp, nxt]
                    else:
                        q = (a4[i + 2] - a4[i]) + (u5[xp, nxt] - u5[xp, prv])
                    p = pltpu.roll(patch_q[at], 127 - 2 * xp, 1)
                    p = jnp.where((ln == 0) | (ln == 127), p, 0.0)
                    out.append((pltpu.roll(q, 127, 1) - pltpu.roll(q, 1, 1)) + p)
                return out

            def finish_half(g, qs, acc):
                at, nxt, prv = group(g), pl.ds(9 + 8 * g, 8), pl.ds(7 + 8 * g, 8)
                dots = []
                for i in range(n):
                    xp = xp0 + i
                    x = v[xp, at]
                    r = ac[xp, at] - (0.5 * mid[xp, at]) * x
                    r = r + (f0[xp, at] * v[xp + 1, at] + f1[xp, at] * v[xp, nxt])
                    r = r + s3[xp, at] * (v[xp + 1, nxt] - v[xp + 1, prv])
                    r = r + (u3[xp + 1, nxt] - u3[xp + 1, prv])
                    r = r + (s4[xp, at] * dz[xp + 1, at] + s5[xp, at] * dz[xp, nxt])
                    dots.append((2.0 * x) * (r + qs[i]))
                return add(acc[0], tree(dots)), acc[1]

            def finish(g, qs, acc):
                if last:
                    return finish_half(g, qs, acc)
                at, nxt, prv = group(g), pl.ds(9 + 8 * g, 8), pl.ds(7 + 8 * g, 8)
                vh = [v[xp0 - 1 + i, at] for i in range(n + 2)]
                vn = [v[xp0 - 1 + i, nxt] for i in range(n + 2)]
                vp = [v[xp0 - 1 + i, prv] for i in range(n + 2)]
                un = [u3[xp0 - 1 + i, nxt] for i in range(n + 2)]
                up = [u3[xp0 - 1 + i, prv] for i in range(n + 2)]
                zh = [dz[xp0 - 1 + i, at] for i in range(n + 2)]
                fx = [f0[xp0 - 1 + i, at] for i in range(n + 1)]
                dots, norms = [], []
                for i in range(n):
                    xp = xp0 + i
                    x = vh[i + 1]
                    r = ac[xp, at] - mid[xp, at] * x
                    r = r + (fx[i + 1] * vh[i + 2] + fx[i] * vh[i])
                    r = r + (f1[xp, at] * vn[i + 1] + f1[xp, prv] * vp[i + 1])
                    r = r + s3[xp, at] * ((vn[i + 2] - vn[i]) - (vp[i + 2] - vp[i]))
                    r = r + ((un[i + 2] - un[i]) - (up[i + 2] - up[i]))
                    r = r + s4[xp, at] * (zh[i + 2] - zh[i])
                    r = r + s5[xp, at] * (dz[xp, nxt] - dz[xp, prv])
                    r = r + qs[i]
                    dots.append(x * r)
                    out = r * inv[xp, at]
                    put(w, xp, g, out)
                    norms.append(out * r)
                if acc is None or g == 8:
                    return acc
                return add(acc[0], tree(dots)), add(acc[1], tree(norms))

            count = 8 if last else 9
            ahead = 2
            pending = [start(g) for g in range(ahead)]
            for g in range(9):
                if g + ahead < count:
                    pending.append(start(g + ahead))
                if then is not None:
                    first(g, [then + i for i in range(4)])
                if g < count:
                    acc = finish(g, pending.pop(0), acc)
            return acc

        def lead(i, carry):
            for g in range(9):
                first(g, [4 * i + 1 + k for k in range(4)])
            return carry

        lax.fori_loop(0, 2, lead, 0)
        out = lax.fori_loop(
            1,
            1 + NX // 4,
            lambda i, acc: second_block(4 * i, 4, acc, 4 * i + 5),
            (none, none),
        )
        if extra:
            lax.fori_loop(
                0,
                2,
                lambda i, c: second_block(4 - extra + (32 + extra) * i, extra, None) or c,
                0,
            )
        return out

    nu1, nu2 = apply(v0, v1, qv0, qv1, 2, False)
    nu3, nu4 = apply(v1, v2, qv1, qv2, 1, False)
    nu5, _ = apply(v2, None, qv2, None, 0, True)

    def store(x, carry):
        w0o[x] = v0[x + 4, OWN]
        w1o[x] = v1[x + 4, OWN]
        w2o[x] = v2[x + 4, OWN]
        return carry

    lax.fori_loop(0, NX, store, 0)
    line = jnp.zeros((1, 128), F32)
    at = iota((1, 128), 1)
    line = jnp.where(at == 6, theta, line)
    for k, (nu, _) in enumerate((nu0, nu1, nu2, nu3, nu4, nu5)):
        part = jnp.sum(jnp.sum(nu, axis=0, keepdims=True), axis=1, keepdims=True)
        line = jnp.where(at == k, part, line)
    mom[...] = jnp.broadcast_to(line, mom.shape)


def combine(mom, w0, w1, w2, out):
    total = jnp.sum(mom[...], axis=0, keepdims=True)
    at = iota((1, 128), 1)
    m = [jnp.sum(jnp.where(at == k, total, 0.0), axis=1, keepdims=True) for k in range(7)]
    rest = 1.0 - m[6] * (1.0 / mom.shape[0])
    a = [rest * m[k] - m[k + 1] for k in range(5)]
    tiny = 1e-7

    def ratio(p, q, limit):
        ok = q > limit
        return jnp.where(ok, p / jnp.where(ok, q, 1.0), 0.0)

    l10 = a[1] / a[0]
    l20 = a[2] / a[0]
    d1 = a[2] - l10 * a[1]
    e12 = a[3] - l10 * a[2]
    g1 = m[1] - l10 * m[0]
    l21 = ratio(e12, d1, tiny * a[2])
    d2 = a[4] - l20 * a[2] - l21 * e12
    g2 = m[2] - l20 * m[0] - l21 * g1
    c2 = ratio(g2, d2, tiny * a[4])
    c1 = ratio(g1, d1, tiny * a[2]) - l21 * c2
    c0 = (m[0] - a[1] * c1 - a[2] * c2) / a[0]

    def plane(x, carry):
        out[x] = c0 * w0[x] + c1 * w1[x] + c2 * w2[x]
        return carry

    lax.fori_loop(0, NX, plane, 0)


def vmem():
    return pl.BlockSpec(memory_space=pltpu.VMEM)


def pack_planes(lab_head, lab_tail, b_head, b_tail, up, down):
    up[pl.ds(0, 3)] = b_head[...]
    up[pl.ds(3, 4)] = lab_head[...].astype(F32)
    down[pl.ds(0, 3)] = b_tail[...]
    down[pl.ds(3, 4)] = lab_tail[...].astype(F32)


def local(labels, conductivity, right_side):
    packet = jax.ShapeDtypeStruct((7, NY, NZ), F32)
    block = jax.ShapeDtypeStruct((NX, NY, NZ), F32)
    xu_own, xl_own = call(pack_planes, 4, [packet] * 2, 4)(
        labels[:4], labels[NX - 4 :], right_side[:3], right_side[NX - 3 :]
    )
    xu = ring(xu_own, "gx", -1)
    xl = ring(xl_own, "gx", 1)

    packet = jax.ShapeDtypeStruct((NX + 8, 8, 128), F32)
    yu_own, yd_own = call(pack_rows, 6, [packet] * 2, 4)(
        labels[:, :8], labels[:, NY - 8 :], right_side[:, :8], right_side[:, NY - 8 :], xu, xl
    )
    yu = ring(yu_own, "gy", -1)
    yd = ring(yd_own, "gy", 1)

    packet = jax.ShapeDtypeStruct((3, 80, 128), F32)
    zu_own, zd_own = call(pack_lanes, 6, [packet] * 2, 6)(labels, right_side, xu, xl, yu, yd)
    zu = ring(zu_own, "gz", -1)
    zd = ring(zd_own, "gz", 1)

    square = pltpu.VMEM((128, 128), F32)
    patch = pltpu.VMEM((80, 128), F32)
    w0, w1, w2, mom = pl.pallas_call(
        sweeps,
        in_specs=[pl.BlockSpec(memory_space=pltpu.SMEM)] + [vmem()] * 10,
        out_specs=[vmem()] * 4,
        out_shape=[block, block, block, jax.ShapeDtypeStruct((128, 128), F32)],
        scratch_shapes=[pltpu.VMEM((XP, RW, 128), F32)] * 17
        + [pltpu.VMEM((XP, 16, 128), F32)] * 19
        + [square, patch, square],
        compiler_params=pltpu.CompilerParams(vmem_limit_bytes=48 * 2**20),
        name="sweeps",
    )(conductivity, labels, right_side, xu, xl, yu, yd, zu_own, zd_own, zu, zd)
    mom = lax.all_to_all(mom, ALL, 0, 0, tiled=True)
    return call(combine, 4, block, 6)(mom, w0, w1, w2)


def call(kernel, inputs, shapes, mib):
    many = isinstance(shapes, list)
    return pl.pallas_call(
        kernel,
        in_specs=[vmem()] * inputs,
        out_specs=[vmem()] * len(shapes) if many else vmem(),
        out_shape=shapes,
        compiler_params=pltpu.CompilerParams(vmem_limit_bytes=mib * 2**20),
        name=kernel.__name__,
    )


def solution(mesh):
    spec = P("gx", "gy", "gz")
    return jax.shard_map(
        local, mesh=mesh, in_specs=(spec, P(), spec), out_specs=spec, check_vma=False
    )
```

```python
import jax
import jax.numpy as jnp
from jax import lax
from jax.experimental import pallas as pl
from jax.experimental.pallas import tpu as pltpu
from jax.sharding import PartitionSpec as P

LABELS = 8
ALL = ("gx", "gy", "gz")
NX, NY, NZ = 32, 64, 128
XP, RW = NX + 10, NY + 24
OWN = slice(8, 8 + NY)
F32 = jnp.float32


def ring(arr, axis, step):
    count = lax.axis_size(axis)
    return lax.ppermute(arr, axis, [(i, (i + step) % count) for i in range(count)])


def iota(shape, dim):
    return lax.broadcasted_iota(jnp.int32, shape, dim)


def pack_rows(lab0, lab7, b0, b7, xu, xl, up, down):
    low = iota((8, 128), 0) < 4
    head, tail = pl.ds(0, 8), pl.ds(NY - 8, 8)

    def put(xp, lab_first, lab_last, b_first, b_last):
        up[xp] = jnp.where(low, b_first, pltpu.roll(lab_first, 4, 0))
        down[xp] = jnp.where(low, pltpu.roll(lab_last, 4, 0), b_last)

    for x in range(NX):
        put(x + 4, lab0[x].astype(F32), lab7[x].astype(F32), b0[x], b7[x])
    zero = jnp.zeros((8, 128), F32)
    for k in range(4):
        bk = (xl[k - 1, head], xl[k - 1, tail]) if k else (zero, zero)
        put(k, xl[3 + k, head], xl[3 + k, tail], *bk)
        bk = (xu[k, head], xu[k, tail]) if k < 3 else (zero, zero)
        put(36 + k, xu[3 + k, head], xu[3 + k, tail], *bk)


def rows_lab(yu, yd, xp):
    low = iota((8, 128), 0) < 4
    return pltpu.roll(jnp.where(low, yd[xp], yu[xp]), 4, 0)


def rows_b(yu, yd, xp):
    low = iota((8, 128), 0) < 4
    return jnp.where(low, yu[xp], yd[xp])


def pack_lanes(lab, b, xu, xl, yu, yd, up, down):
    lane = iota((8, 128), 1)
    first = lane % 8 < 4
    zero = jnp.zeros((8, 128), F32)

    def pack(at, lab_of, b_of):
        for g in range(3):
            acc_lab, acc_b = zero, zero
            for k in range(16 if g < 2 else 8):
                hit = lane // 8 == k
                shift = (8 * k + 4) % 128
                turn = lambda t: pltpu.roll(t, shift, 1) if shift else t
                acc_lab = jnp.where(hit, turn(lab_of(16 * g + k)), acc_lab)
                acc_b = jnp.where(hit, turn(b_of(16 * g + k)), acc_b)
            for off in at:
                down[g, off] = jnp.where(first, acc_lab, pltpu.roll(acc_b, 4, 1))
                up[g, off] = jnp.where(first, pltpu.roll(acc_b, 124, 1), acc_lab)

    def rows(rg, carry):
        at = pl.ds(pl.multiple_of(8 * rg, 8), 8)

        def lab_of(xp):
            if xp < 4:
                return xl[3 + xp, at]
            if xp >= 36:
                return xu[xp - 33, at]
            return lab[xp - 4, at].astype(F32)

        def b_of(xp):
            if xp < 4:
                return xl[xp - 1, at] if xp else zero
            if xp >= 36:
                return xu[xp - 36, at] if xp < 39 else zero
            return b[xp - 4, at]

        pack((pl.ds(pl.multiple_of(8 * rg + 8, 8), 8),), lab_of, b_of)
        return carry

    lax.fori_loop(0, 8, rows, 0)
    pack(
        (pl.ds(0, 8), pl.ds(72, 8)),
        lambda xp: rows_lab(yu, yd, xp),
        lambda xp: rows_b(yu, yd, xp),
    )


def group(g):
    return pl.ds(8 + 8 * g, 8)


def grid_flags():
    first, last = [], []
    for axis in ALL:
        at = lax.axis_index(axis)
        first.append((at > 0).astype(F32))
        last.append((at < lax.axis_size(axis) - 1).astype(F32))
    return first, last


def entries_of(cond):
    sub8 = iota((8, 128), 0)
    tables = []
    for c in range(7):
        t = jnp.zeros((8, 128), F32)
        scale = 0.5 if c < 3 else (0.25 if c < 6 else 1.0)
        for l in range(LABELS):
            t = jnp.where(sub8 == l, cond[c, l] * scale, t)
        tables.append(t)

    def look(c, idx):
        return jnp.take_along_axis(tables[c], idx, axis=0, mode="promise_in_bounds")

    def entries(idx, on):
        vals = [look(c, idx) for c in range(7)]
        if on is not None:
            vals = [v * on for v in vals]
        centre = vals[6] + 2.0 * (vals[0] + vals[1] + vals[2])
        return vals[:6], centre

    return entries


def put(ref, xp, g, value):
    ref[xp, group(g)] = value
    if g == 8:
        ref[xp, pl.ds(0, 8)] = value
    if g == 0:
        ref[xp, pl.ds(80, 8)] = value


def blocks(body, extra, sums):
    if extra:
        lax.fori_loop(
            0, 2, lambda i, c: body(4 - extra + (32 + extra) * i, extra, None) or c, 0
        )
    return lax.fori_loop(0, NX // 4, lambda i, acc: body(4 * i + 4, 4, acc), sums)


OUTSIDE = 1e30


def faces(cond, lab, b, xu, xl, yu, yd, f0, f1, diag, s2, s3, s4, s5, v0, s0, s1):
    sig = (s0, s1, s2, s3, s4, s5)
    (not_first_x, not_first_y, _), (not_last_x, not_last_y, _) = grid_flags()
    entries = entries_of(cond)
    sub8 = iota((8, 128), 0)
    row_on = jnp.where(sub8 < 4, not_last_y, not_first_y)

    def table_plane(xp, labels_of, b_of, on):
        for g in range(9):
            if g < 8:
                vals, centre = entries(labels_of(g), on)
                v0[xp, group(g)] = b_of(g)
            else:
                vals, centre = entries(
                    rows_lab(yu, yd, xp).astype(jnp.int32),
                    row_on if on is None else row_on * on,
                )
                v0[xp, group(g)] = rows_b(yu, yd, xp)
            for c in range(6):
                if c == 1:
                    put(s1, xp, g, vals[1])
                else:
                    sig[c][xp, group(g)] = vals[c]
            diag[xp, group(g)] = centre

    def own_plane(x, carry):
        table_plane(
            x + 4, lambda g: lab[x, pl.ds(8 * g, 8)], lambda g: b[x, pl.ds(8 * g, 8)], None
        )
        return carry

    lax.fori_loop(0, NX, own_plane, 0)

    def low_plane(k, carry):
        table_plane(
            k,
            lambda g: xl[3 + k, pl.ds(8 * g, 8)].astype(jnp.int32),
            lambda g: xl[jnp.maximum(k - 1, 0), pl.ds(8 * g, 8)],
            not_first_x,
        )
        return carry

    def high_plane(k, carry):
        table_plane(
            36 + k,
            lambda g: xu[3 + k, pl.ds(8 * g, 8)].astype(jnp.int32),
            lambda g: xu[jnp.minimum(k, 2), pl.ds(8 * g, 8)],
            not_last_x,
        )
        return carry

    lax.fori_loop(0, 4, low_plane, 0)
    lax.fori_loop(0, 4, high_plane, 0)

    def sums(xp0, n, acc):
        for g in range(9):
            at, nxt, prv = group(g), pl.ds(9 + 8 * g, 8), pl.ds(7 + 8 * g, 8)
            across = [s0[xp0 - 1 + i, at] for i in range(n + 2)]
            for i in range(n):
                xp = xp0 + i
                c = diag[xp, at]
                up = s1[xp, nxt]
                total = c + (across[i + 2] + across[i]) + (up + s1[xp, prv])
                diag[xp, at] = jnp.where(c > 0, total, OUTSIDE)
                f0[xp, at] = across[i + 1] + across[i + 2]
                put(f1, xp, g, s1[xp, at] + up)
        return acc

    blocks(sums, 3, 0)


def sweeps(
    cond, f0, f1, diag, s2, s3, s4, s5, rhs, zu_own, zd_own, zu, zd,
    w0o, w1o, w2o, mom,
    f2, f2l, inv, mid, v0, v1, v2, dz, ac, u3, u4, u5,
    q0, q1, q2, q3, q4, q5, qf1, qf1l, qf2, qf2l, qinv, qmid, qv0, qv1, qv2,
    qdy, p3, p4, p5,
    wide, patch_q, row_q,
):
    qsig = (q0, q1, q2, q3, q4, q5)
    (not_first_x, not_first_y, not_first_z), (not_last_x, not_last_y, not_last_z) = grid_flags()
    entries = entries_of(cond)
    sub8 = iota((8, 128), 0)
    ln = iota((8, 128), 1)

    mass = sum(cond[6, l] for l in range(LABELS))
    faces = sum(cond[c, l] for c in range(3) for l in range(LABELS)) * 2.0
    theta = jnp.full((1, 128), faces, F32) / jnp.full((1, 128), faces + mass, F32)

    first = iota((80, 128), 1) % 8 < 4
    wide[...] = jnp.zeros((128, 128), F32)
    lane_on = jnp.where(ln < 8, not_first_y, jnp.where(ln >= 72, not_last_y, 1.0))
    low_on = jnp.where(sub8 < 4, not_first_z, 1.0) * lane_on
    high_on = jnp.where(sub8 < 4, 1.0, not_last_z) * lane_on

    def turned(arr):
        wide[pl.ds(0, 80)] = arr
        return wide[...].T

    for g in range(3):
        count = 16 if g < 2 else 8
        parts = (
            (0, low_on, turned(jnp.where(first, zd[g], zu_own[g])),
             turned(jnp.where(first, zu_own[g], zd[g]))),
            (8, high_on, turned(jnp.where(first, zd_own[g], zu[g])),
             turned(jnp.where(first, zu[g], zd_own[g]))),
        )
        for off, on, labs, bs in parts:
            for k in range(count):
                xp = 16 * g + k
                here = on
                if xp < 4:
                    here = on * not_first_x
                if xp >= 36:
                    here = on * not_last_x
                idx = jnp.clip(labs[8 * k : 8 * k + 8].astype(jnp.int32), 0, LABELS - 1)
                vals, centre = entries(idx, here)
                for c in range(6):
                    qsig[c][xp + 1, pl.ds(off, 8)] = vals[c]
                qinv[xp + 1, pl.ds(off, 8)] = centre
                qv0[xp + 1, pl.ds(off, 8)] = pltpu.roll(bs[8 * k : 8 * k + 8], 4, 0)

    def set_rows(ref, xp, for_first, for_last):
        for k in range(QB):
            ref[pl.ds(2 * (xp + k) + 1, 1)] = for_first[k]
            ref[pl.ds(2 * (xp + k), 1)] = for_last[k]

    def set_patch(patch, rows):
        t = rows[...].T
        patch[...] = t[:80]
        patch[pl.ds(72, 8)] = jnp.where(sub8 < 4, t[72:80], t[:8])

    def sides(value, patch, xp, g):
        p = pltpu.roll(patch[group(g)], 127 - 2 * xp, 1)
        left = jnp.where(ln == 0, p, pltpu.roll(value, 1, 1))
        right = jnp.where(ln == 127, p, pltpu.roll(value, 127, 1))
        return left, right

    QB = 8

    def q_loop(body):
        lax.fori_loop(0, (NX + 8) // QB, lambda i, c: body(QB * i) or c, 0)

    def lanes(x, step):
        return pltpu.roll(x, step % 128, 2)

    def subs(x, step):
        return pltpu.roll(x, step % 16, 1)

    row_q[...] = jnp.zeros((128, 128), F32)

    def reciprocal(centre, total):
        return jnp.where(centre > 0, 1.0 / jnp.where(centre > 0, total, 1.0), 0.0)

    def q_diag(xp):
        at = pl.ds(xp + 1, QB)
        c = qinv[at]
        b1 = q1[at]
        b2 = q2[at]
        r1, l1 = lanes(b1, -1), lanes(b1, 1)
        r2, l2 = subs(b2, -1), subs(b2, 1)
        total = c + (q0[pl.ds(xp + 2, QB)] + q0[pl.ds(xp, QB)])
        total = total + (l1 + r1)
        total = total + (l2 + r2)
        qf1[at] = b1 + r1
        qf1l[at] = b1 + l1
        qf2[at] = b2 + r2
        qf2l[at] = b2 + l2
        r = reciprocal(c, total)
        qinv[at] = r
        qmid[at] = theta * total
        w = qv0[at] * r
        qv0[at] = w
        set_rows(row_q, xp, b2[:, 3:4], b2[:, 12:13])

    q_loop(q_diag)
    set_patch(patch_q, row_q)

    def add(acc, value):
        total, lost = acc
        value = value - lost
        new = total + value
        return new, (new - total) - value

    def tree(values):
        while len(values) > 1:
            values = [sum(values[i : i + 2]) for i in range(0, len(values), 2)]
        return values[0]

    zero8 = jnp.zeros((8, 128), F32)
    none = (zero8, zero8)

    def diag_block(xp0, n, acc):
        for g in range(9):
            at = group(g)
            parts = []
            for xp in [xp0 + i for i in range(n)]:
                a2 = s2[xp, at]
                left, right = sides(a2, patch_q, xp, g)
                total = diag[xp, at]
                inside = total < 0.5 * OUTSIDE
                total = total + (left + right)
                r = jnp.where(inside, 1.0 / total, 0.0)
                b = rhs[xp, at]
                w = b * r
                inv[xp, at] = r
                mid[xp, at] = jnp.where(inside, theta * total, 0.0)
                put(v0, xp, g, w)
                f2[xp, at] = a2 + right
                f2l[xp, at] = a2 + left
                parts.append(b * w)
            if acc is not None and g < 8:
                acc = add(acc, tree(parts))
        return acc

    nu0 = blocks(diag_block, 3, none)

    def apply(v, w, qv, qw, extra, last):
        def q_first(xp):
            at = pl.ds(xp + 1, QB)
            x = qv[at]
            p4[at] = q4[at] * x
            p5[at] = q5[at] * x
            if not last:
                right, left = lanes(x, -1), lanes(x, 1)
                qdy[at] = right - left
                p3[at] = q3[at] * x
                r = qf2[at] * subs(x, -1) + qf2l[at] * subs(x, 1)
                r = r + (qf1[at] * right + qf1l[at] * left)
                qw[at] = r - qmid[at] * x

        q_loop(q_first)

        def q_second(xp):
            at, nx, pr = pl.ds(xp + 1, QB), pl.ds(xp + 2, QB), pl.ds(xp, QB)
            xa, x5 = qv[nx], p5[at]
            if not last:
                xb = qv[pr]
                dx = xa - xb
                dx4 = p4[nx] - p4[pr]
                y = qdy[at]
            x = qv[at]
            if last:
                q = p4[nx] + lanes(x5, -1)
                e, ex, eq = (t[:, :8] - t[:, 8:] for t in (x, xa, q))
                ey = pltpu.roll(e, 127, 2)
            else:
                q = dx4 + (lanes(x5, -1) - lanes(x5, 1))
                e, ex, ey, eq = (t[:, :8] - t[:, 8:] for t in (x, dx, y, q))

            def turn(t, step):
                return pltpu.roll(t, step % 8, 1)

            b4, b5 = q4[at], q5[at]
            first = -(b4[:, :8] * turn(ex, 1) + b5[:, :8] * turn(ey, 1)) - turn(eq, 1)
            if not last:
                first = first + qf2l[at][:, :8] * turn(e, 1)
            final = qf2[at][:, 8:] * turn(e, -1) + b4[:, 8:] * turn(ex, -1)
            final = final + b5[:, 8:] * turn(ey, -1) + turn(eq, -1)
            set_rows(row_q, xp, first[:, 4:5], -final[:, 3:4])
            if not last:
                b0 = q0[at]
                t = (p3[nx] - p3[pr]) + (subs(x5, -1) - subs(x5, 1))
                r = qw[at] + (b0 + q0[nx]) * xa + (b0 + q0[pr]) * xb
                r = r + (lanes(t, -1) - lanes(t, 1))
                r = r + q3[at] * (qdy[nx] - qdy[pr])
                r = r + b4 * (subs(dx, -1) - subs(dx, 1))
                r = r + b5 * (subs(y, -1) - subs(y, 1))
                r = r + (subs(dx4, -1) - subs(dx4, 1))
                qw[at] = r * qinv[at]

        q_loop(q_second)
        set_patch(patch_q, row_q)

        def first(g, xps):
            at = group(g)
            for xp in xps:
                x = v[xp, at]
                left, right = pltpu.roll(x, 1, 1), pltpu.roll(x, 127, 1)
                put(dz, xp, g, right - left)
                if last:
                    ac[xp, at] = f2[xp, at] * right
                else:
                    ac[xp, at] = f2[xp, at] * right + f2l[xp, at] * left
                put(u3, xp, g, s3[xp, at] * x)
                u4[xp, at] = s4[xp, at] * x
                put(u5, xp, g, s5[xp, at] * x)

        def second_block(xp0, n, acc, then=None):
            def start(g):
                at, nxt, prv = group(g), pl.ds(9 + 8 * g, 8), pl.ds(7 + 8 * g, 8)
                a4 = [u4[xp0 - 1 + i, at] for i in range(n + 2)]
                out = []
                for i in range(n):
                    xp = xp0 + i
                    if last:
                        q = a4[i + 2] + u5[xp, nxt]
                    else:
                        q = (a4[i + 2] - a4[i]) + (u5[xp, nxt] - u5[xp, prv])
                    p = pltpu.roll(patch_q[at], 127 - 2 * xp, 1)
                    p = jnp.where((ln == 0) | (ln == 127), p, 0.0)
                    out.append((pltpu.roll(q, 127, 1) - pltpu.roll(q, 1, 1)) + p)
                return out

            def finish_half(g, qs, acc):
                at, nxt, prv = group(g), pl.ds(9 + 8 * g, 8), pl.ds(7 + 8 * g, 8)
                dots = []
                for i in range(n):
                    xp = xp0 + i
                    x = v[xp, at]
                    r = ac[xp, at] - (0.5 * mid[xp, at]) * x
                    r = r + (f0[xp, at] * v[xp + 1, at] + f1[xp, at] * v[xp, nxt])
                    r = r + s3[xp, at] * (v[xp + 1, nxt] - v[xp + 1, prv])
                    r = r + (u3[xp + 1, nxt] - u3[xp + 1, prv])
                    r = r + (s4[xp, at] * dz[xp + 1, at] + s5[xp, at] * dz[xp, nxt])
                    dots.append((2.0 * x) * (r + qs[i]))
                return add(acc[0], tree(dots)), acc[1]

            def finish(g, qs, acc):
                if last:
                    return finish_half(g, qs, acc)
                at, nxt, prv = group(g), pl.ds(9 + 8 * g, 8), pl.ds(7 + 8 * g, 8)
                vh = [v[xp0 - 1 + i, at] for i in range(n + 2)]
                vn = [v[xp0 - 1 + i, nxt] for i in range(n + 2)]
                vp = [v[xp0 - 1 + i, prv] for i in range(n + 2)]
                un = [u3[xp0 - 1 + i, nxt] for i in range(n + 2)]
                up = [u3[xp0 - 1 + i, prv] for i in range(n + 2)]
                zh = [dz[xp0 - 1 + i, at] for i in range(n + 2)]
                fx = [f0[xp0 - 1 + i, at] for i in range(n + 1)]
                dots, norms = [], []
                for i in range(n):
                    xp = xp0 + i
                    x = vh[i + 1]
                    r = ac[xp, at] - mid[xp, at] * x
                    r = r + (fx[i + 1] * vh[i + 2] + fx[i] * vh[i])
                    r = r + (f1[xp, at] * vn[i + 1] + f1[xp, prv] * vp[i + 1])
                    r = r + s3[xp, at] * ((vn[i + 2] - vn[i]) - (vp[i + 2] - vp[i]))
                    r = r + ((un[i + 2] - un[i]) - (up[i + 2] - up[i]))
                    r = r + s4[xp, at] * (zh[i + 2] - zh[i])
                    r = r + s5[xp, at] * (dz[xp, nxt] - dz[xp, prv])
                    r = r + qs[i]
                    dots.append(x * r)
                    out = r * inv[xp, at]
                    put(w, xp, g, out)
                    norms.append(out * r)
                if acc is None or g == 8:
                    return acc
                return add(acc[0], tree(dots)), add(acc[1], tree(norms))

            count = 8 if last else 9
            ahead = 2
            pending = [start(g) for g in range(ahead)]
            for g in range(9):
                if g + ahead < count:
                    pending.append(start(g + ahead))
                if then is not None:
                    first(g, [then + i for i in range(4)])
                if g < count:
                    acc = finish(g, pending.pop(0), acc)
            return acc

        def lead(i, carry):
            for g in range(9):
                first(g, [4 * i + 1 + k for k in range(4)])
            return carry

        lax.fori_loop(0, 2, lead, 0)
        out = lax.fori_loop(
            1,
            1 + NX // 4,
            lambda i, acc: second_block(4 * i, 4, acc, 4 * i + 5),
            (none, none),
        )
        if extra:
            lax.fori_loop(
                0,
                2,
                lambda i, c: second_block(4 - extra + (32 + extra) * i, extra, None) or c,
                0,
            )
        return out

    nu1, nu2 = apply(v0, v1, qv0, qv1, 2, False)
    nu3, nu4 = apply(v1, v2, qv1, qv2, 1, False)
    nu5, _ = apply(v2, None, qv2, None, 0, True)

    def store(x, carry):
        w0o[x] = v0[x + 4, OWN]
        w1o[x] = v1[x + 4, OWN]
        w2o[x] = v2[x + 4, OWN]
        return carry

    lax.fori_loop(0, NX, store, 0)
    line = jnp.zeros((1, 128), F32)
    at = iota((1, 128), 1)
    line = jnp.where(at == 6, theta, line)
    for k, (nu, _) in enumerate((nu0, nu1, nu2, nu3, nu4, nu5)):
        part = jnp.sum(jnp.sum(nu, axis=0, keepdims=True), axis=1, keepdims=True)
        line = jnp.where(at == k, part, line)
    mom[...] = jnp.broadcast_to(line, mom.shape)


def combine(mom, w0, w1, w2, out):
    total = jnp.sum(mom[...], axis=0, keepdims=True)
    at = iota((1, 128), 1)
    m = [jnp.sum(jnp.where(at == k, total, 0.0), axis=1, keepdims=True) for k in range(7)]
    rest = 1.0 - m[6] * (1.0 / mom.shape[0])
    a = [rest * m[k] - m[k + 1] for k in range(5)]
    tiny = 1e-7

    def ratio(p, q, limit):
        ok = q > limit
        return jnp.where(ok, p / jnp.where(ok, q, 1.0), 0.0)

    l10 = a[1] / a[0]
    l20 = a[2] / a[0]
    d1 = a[2] - l10 * a[1]
    e12 = a[3] - l10 * a[2]
    g1 = m[1] - l10 * m[0]
    l21 = ratio(e12, d1, tiny * a[2])
    d2 = a[4] - l20 * a[2] - l21 * e12
    g2 = m[2] - l20 * m[0] - l21 * g1
    c2 = ratio(g2, d2, tiny * a[4])
    c1 = ratio(g1, d1, tiny * a[2]) - l21 * c2
    c0 = (m[0] - a[1] * c1 - a[2] * c2) / a[0]

    def plane(x, carry):
        out[x] = c0 * w0[x] + c1 * w1[x] + c2 * w2[x]
        return carry

    lax.fori_loop(0, NX, plane, 0)


def vmem():
    return pl.BlockSpec(memory_space=pltpu.VMEM)


def pack_planes(lab_head, lab_tail, b_head, b_tail, up, down):
    up[pl.ds(0, 3)] = b_head[...]
    up[pl.ds(3, 4)] = lab_head[...].astype(F32)
    down[pl.ds(0, 3)] = b_tail[...]
    down[pl.ds(3, 4)] = lab_tail[...].astype(F32)


def local(labels, conductivity, right_side):
    packet = jax.ShapeDtypeStruct((7, NY, NZ), F32)
    block = jax.ShapeDtypeStruct((NX, NY, NZ), F32)
    xu_own, xl_own = call(pack_planes, 4, [packet] * 2, 4)(
        labels[:4], labels[NX - 4 :], right_side[:3], right_side[NX - 3 :]
    )
    xu = ring(xu_own, "gx", -1)
    xl = ring(xl_own, "gx", 1)

    packet = jax.ShapeDtypeStruct((NX + 8, 8, 128), F32)
    yu_own, yd_own = call(pack_rows, 6, [packet] * 2, 4)(
        labels[:, :8], labels[:, NY - 8 :], right_side[:, :8], right_side[:, NY - 8 :], xu, xl
    )
    yu = ring(yu_own, "gy", -1)
    yd = ring(yd_own, "gy", 1)

    packet = jax.ShapeDtypeStruct((3, 80, 128), F32)
    zu_own, zd_own = call(pack_lanes, 6, [packet] * 2, 6)(labels, right_side, xu, xl, yu, yd)
    zu = ring(zu_own, "gz", -1)
    zd = ring(zd_own, "gz", 1)

    square = pltpu.VMEM((128, 128), F32)
    patch = pltpu.VMEM((80, 128), F32)
    main = (XP, RW, 128)
    tables = pl.pallas_call(
        faces,
        in_specs=[pl.BlockSpec(memory_space=pltpu.SMEM)] + [vmem()] * 6,
        out_specs=[vmem()] * 8,
        out_shape=[jax.ShapeDtypeStruct(main, F32)] * 8,
        scratch_shapes=[pltpu.VMEM(main, F32)] * 2,
        compiler_params=pltpu.CompilerParams(vmem_limit_bytes=5 * 2**20),
        cost_estimate=pl.CostEstimate(flops=8 * 10**6, bytes_accessed=0, transcendentals=0),
        name="faces",
    )(conductivity, labels, right_side, xu, xl, yu, yd)
    w0, w1, w2, mom = pl.pallas_call(
        sweeps,
        in_specs=[pl.BlockSpec(memory_space=pltpu.SMEM)] + [vmem()] * 12,
        out_specs=[vmem()] * 4,
        out_shape=[block, block, block, jax.ShapeDtypeStruct((128, 128), F32)],
        scratch_shapes=[pltpu.VMEM(main, F32)] * 12
        + [pltpu.VMEM((XP, 16, 128), F32)] * 19
        + [square, patch, square],
        compiler_params=pltpu.CompilerParams(vmem_limit_bytes=33 * 2**20),
        name="sweeps",
    )(conductivity, *tables, zu_own, zd_own, zu, zd)
    mom = lax.all_to_all(mom, ALL, 0, 0, tiled=True)
    return call(combine, 4, block, 6)(mom, w0, w1, w2)


def call(kernel, inputs, shapes, mib):
    many = isinstance(shapes, list)
    return pl.pallas_call(
        kernel,
        in_specs=[vmem()] * inputs,
        out_specs=[vmem()] * len(shapes) if many else vmem(),
        out_shape=shapes,
        compiler_params=pltpu.CompilerParams(vmem_limit_bytes=mib * 2**20),
        name=kernel.__name__,
    )


def solution(mesh):
    spec = P("gx", "gy", "gz")
    return jax.shard_map(
        local, mesh=mesh, in_specs=(spec, P(), spec), out_specs=spec, check_vma=False
    )
```

```python
import jax
import jax.numpy as jnp
from jax import lax
from jax.experimental import pallas as pl
from jax.experimental.pallas import tpu as pltpu
from jax.sharding import PartitionSpec as P

LABELS = 8
ALL = ("gx", "gy", "gz")
NX, NY, NZ = 32, 64, 128
XP, RW = NX + 10, NY + 24
OWN = slice(8, 8 + NY)
F32 = jnp.float32


def ring(arr, axis, step):
    count = lax.axis_size(axis)
    return lax.ppermute(arr, axis, [(i, (i + step) % count) for i in range(count)])


def iota(shape, dim):
    return lax.broadcasted_iota(jnp.int32, shape, dim)


def pack_rows(lab0, lab7, b0, b7, xu, xl, up, down):
    low = iota((8, 128), 0) < 4
    head, tail = pl.ds(0, 8), pl.ds(NY - 8, 8)

    def put(xp, lab_first, lab_last, b_first, b_last):
        up[xp] = jnp.where(low, b_first, pltpu.roll(lab_first, 4, 0))
        down[xp] = jnp.where(low, pltpu.roll(lab_last, 4, 0), b_last)

    for x in range(NX):
        put(x + 4, lab0[x].astype(F32), lab7[x].astype(F32), b0[x], b7[x])
    zero = jnp.zeros((8, 128), F32)
    for k in range(4):
        bk = (xl[k - 1, head], xl[k - 1, tail]) if k else (zero, zero)
        put(k, xl[3 + k, head], xl[3 + k, tail], *bk)
        bk = (xu[k, head], xu[k, tail]) if k < 3 else (zero, zero)
        put(36 + k, xu[3 + k, head], xu[3 + k, tail], *bk)


def rows_lab(yu, yd, xp):
    low = iota((8, 128), 0) < 4
    return pltpu.roll(jnp.where(low, yd[xp], yu[xp]), 4, 0)


def rows_b(yu, yd, xp):
    low = iota((8, 128), 0) < 4
    return jnp.where(low, yu[xp], yd[xp])


def gather(lane, planes, of, g, acc):
    for xp in planes:
        if xp // 16 != g:
            continue
        k = xp % 16
        shift = (8 * k + 4) % 128
        value = of(xp)
        acc = jnp.where(lane // 8 == k, pltpu.roll(value, shift, 1) if shift else value, acc)
    return acc


def pack_own(lab, b, lab_part, b_part):
    lane = iota((8, 128), 1)
    zero = jnp.zeros((8, 128), F32)

    def rows(rg, carry):
        at = pl.ds(pl.multiple_of(8 * rg, 8), 8)
        own = range(4, NX + 4)
        for g in range(3):
            lab_part[g, at] = gather(lane, own, lambda xp: lab[xp - 4, at].astype(F32), g, zero)
            b_part[g, at] = gather(lane, own, lambda xp: b[xp - 4, at], g, zero)
        return carry

    lax.fori_loop(0, NY // 8, rows, 0)


def pack_lanes(lab_part, b_part, xu, xl, yu, yd, up, down):
    lane = iota((8, 128), 1)
    first = lane % 8 < 4
    zero = jnp.zeros((8, 128), F32)

    def send(g, at, lab, b):
        down[g, at] = jnp.where(first, lab, pltpu.roll(b, 4, 1))
        up[g, at] = jnp.where(first, pltpu.roll(b, 124, 1), lab)

    everything = range(NX + 8)
    beside = [xp for xp in everything if xp < 4 or xp >= NX + 4]
    for g in range(3):
        lab = gather(lane, everything, lambda xp: rows_lab(yu, yd, xp), g, zero)
        b = gather(lane, everything, lambda xp: rows_b(yu, yd, xp), g, zero)
        send(g, pl.ds(0, 8), lab, b)
        send(g, pl.ds(72, 8), lab, b)
        for rg in range(NY // 8):
            at = pl.ds(8 * rg, 8)

            def lab_of(xp):
                return xl[3 + xp, at] if xp < 4 else xu[xp - 33, at]

            def b_of(xp):
                if xp < 4:
                    return xl[xp - 1, at] if xp else zero
                return xu[xp - 36, at] if xp < 39 else zero

            lab = gather(lane, beside, lab_of, g, lab_part[g, at])
            b = gather(lane, beside, b_of, g, b_part[g, at])
            send(g, group(rg), lab, b)


def group(g):
    return pl.ds(8 + 8 * g, 8)


def grid_flags():
    first, last = [], []
    for axis in ALL:
        at = lax.axis_index(axis)
        first.append((at > 0).astype(F32))
        last.append((at < lax.axis_size(axis) - 1).astype(F32))
    return first, last


def entries_of(cond):
    sub8 = iota((8, 128), 0)
    tables = []
    for c in range(7):
        t = jnp.zeros((8, 128), F32)
        scale = 0.5 if c < 3 else (0.25 if c < 6 else 1.0)
        for l in range(LABELS):
            t = jnp.where(sub8 == l, cond[c, l] * scale, t)
        tables.append(t)

    def look(c, idx):
        return jnp.take_along_axis(tables[c], idx, axis=0, mode="promise_in_bounds")

    def entries(idx, on):
        vals = [look(c, idx) for c in range(7)]
        if on is not None:
            vals = [v * on for v in vals]
        centre = vals[6] + 2.0 * (vals[0] + vals[1] + vals[2])
        return vals[:6], centre

    return entries


def put(ref, xp, g, value):
    ref[xp, group(g)] = value
    if g == 8:
        ref[xp, pl.ds(0, 8)] = value
    if g == 0:
        ref[xp, pl.ds(80, 8)] = value


def blocks(body, extra, sums):
    if extra:
        lax.fori_loop(
            0, 2, lambda i, c: body(4 - extra + (32 + extra) * i, extra, None) or c, 0
        )
    return lax.fori_loop(0, NX // 4, lambda i, acc: body(4 * i + 4, 4, acc), sums)


OUTSIDE = 1e30


def faces(cond, lab, b, xu, xl, yu, yd, f0, f1, diag, s2, s3, s4, s5, v0, s0, s1):
    sig = (s0, s1, s2, s3, s4, s5)
    (not_first_x, not_first_y, _), (not_last_x, not_last_y, _) = grid_flags()
    entries = entries_of(cond)
    sub8 = iota((8, 128), 0)
    row_on = jnp.where(sub8 < 4, not_last_y, not_first_y)

    def table_plane(xp, labels_of, b_of, on):
        for g in range(9):
            if g < 8:
                vals, centre = entries(labels_of(g), on)
                v0[xp, group(g)] = b_of(g)
            else:
                vals, centre = entries(
                    rows_lab(yu, yd, xp).astype(jnp.int32),
                    row_on if on is None else row_on * on,
                )
                v0[xp, group(g)] = rows_b(yu, yd, xp)
            for c in range(6):
                if c == 1:
                    put(s1, xp, g, vals[1])
                else:
                    sig[c][xp, group(g)] = vals[c]
            diag[xp, group(g)] = centre

    def own_plane(x, carry):
        table_plane(
            x + 4, lambda g: lab[x, pl.ds(8 * g, 8)], lambda g: b[x, pl.ds(8 * g, 8)], None
        )
        return carry

    lax.fori_loop(0, NX, own_plane, 0)

    def low_plane(k, carry):
        table_plane(
            k,
            lambda g: xl[3 + k, pl.ds(8 * g, 8)].astype(jnp.int32),
            lambda g: xl[jnp.maximum(k - 1, 0), pl.ds(8 * g, 8)],
            not_first_x,
        )
        return carry

    def high_plane(k, carry):
        table_plane(
            36 + k,
            lambda g: xu[3 + k, pl.ds(8 * g, 8)].astype(jnp.int32),
            lambda g: xu[jnp.minimum(k, 2), pl.ds(8 * g, 8)],
            not_last_x,
        )
        return carry

    lax.fori_loop(0, 4, low_plane, 0)
    lax.fori_loop(0, 4, high_plane, 0)

    def sums(xp0, n, acc):
        for g in range(9):
            at, nxt, prv = group(g), pl.ds(9 + 8 * g, 8), pl.ds(7 + 8 * g, 8)
            across = [s0[xp0 - 1 + i, at] for i in range(n + 2)]
            for i in range(n):
                xp = xp0 + i
                c = diag[xp, at]
                up = s1[xp, nxt]
                total = c + (across[i + 2] + across[i]) + (up + s1[xp, prv])
                diag[xp, at] = jnp.where(c > 0, total, OUTSIDE)
                f0[xp, at] = across[i + 1] + across[i + 2]
                put(f1, xp, g, s1[xp, at] + up)
        return acc

    blocks(sums, 3, 0)


def sweeps(
    cond, f0, f1, diag, s2, s3, s4, s5, rhs, zu_own, zd_own, zu, zd,
    w0o, w1o, w2o, mom,
    f2, f2l, inv, mid, v0, v1, v2, dz, ac, u3, u4, u5,
    q0, q1, q2, q3, q4, q5, qf1, qf1l, qf2, qf2l, qinv, qmid, qv0, qv1, qv2,
    qdy, p3, p4, p5,
    wide, patch_q, row_q,
):
    qsig = (q0, q1, q2, q3, q4, q5)
    (not_first_x, not_first_y, not_first_z), (not_last_x, not_last_y, not_last_z) = grid_flags()
    entries = entries_of(cond)
    sub8 = iota((8, 128), 0)
    ln = iota((8, 128), 1)

    mass = sum(cond[6, l] for l in range(LABELS))
    faces = sum(cond[c, l] for c in range(3) for l in range(LABELS)) * 2.0
    theta = jnp.full((1, 128), faces, F32) / jnp.full((1, 128), faces + mass, F32)

    first = iota((80, 128), 1) % 8 < 4
    wide[...] = jnp.zeros((128, 128), F32)
    lane_on = jnp.where(ln < 8, not_first_y, jnp.where(ln >= 72, not_last_y, 1.0))
    low_on = jnp.where(sub8 < 4, not_first_z, 1.0) * lane_on
    high_on = jnp.where(sub8 < 4, 1.0, not_last_z) * lane_on

    def turned(arr):
        wide[pl.ds(0, 80)] = arr
        return wide[...].T

    for g in range(3):
        count = 16 if g < 2 else 8
        parts = (
            (0, low_on, turned(jnp.where(first, zd[g], zu_own[g])),
             turned(jnp.where(first, zu_own[g], zd[g]))),
            (8, high_on, turned(jnp.where(first, zd_own[g], zu[g])),
             turned(jnp.where(first, zu[g], zd_own[g]))),
        )
        for off, on, labs, bs in parts:
            for k in range(count):
                xp = 16 * g + k
                here = on
                if xp < 4:
                    here = on * not_first_x
                if xp >= 36:
                    here = on * not_last_x
                idx = jnp.clip(labs[8 * k : 8 * k + 8].astype(jnp.int32), 0, LABELS - 1)
                vals, centre = entries(idx, here)
                for c in range(6):
                    qsig[c][xp + 1, pl.ds(off, 8)] = vals[c]
                qinv[xp + 1, pl.ds(off, 8)] = centre
                qv0[xp + 1, pl.ds(off, 8)] = pltpu.roll(bs[8 * k : 8 * k + 8], 4, 0)

    def set_rows(ref, xp, for_first, for_last):
        for k in range(QB):
            ref[pl.ds(2 * (xp + k) + 1, 1)] = for_first[k]
            ref[pl.ds(2 * (xp + k), 1)] = for_last[k]

    def set_patch(patch, rows):
        t = rows[...].T
        patch[...] = t[:80]
        patch[pl.ds(72, 8)] = jnp.where(sub8 < 4, t[72:80], t[:8])

    def sides(value, patch, xp, g):
        p = pltpu.roll(patch[group(g)], 127 - 2 * xp, 1)
        left = jnp.where(ln == 0, p, pltpu.roll(value, 1, 1))
        right = jnp.where(ln == 127, p, pltpu.roll(value, 127, 1))
        return left, right

    QB = 40

    def q_loop(body):
        lax.fori_loop(0, (NX + 8) // QB, lambda i, c: body(QB * i) or c, 0)

    def lanes(x, step):
        return pltpu.roll(x, step % 128, 2)

    def subs(x, step):
        return pltpu.roll(x, step % 16, 1)

    row_q[...] = jnp.zeros((128, 128), F32)

    def reciprocal(centre, total):
        return jnp.where(centre > 0, 1.0 / jnp.where(centre > 0, total, 1.0), 0.0)

    def q_diag(xp):
        at = pl.ds(xp + 1, QB)
        c = qinv[at]
        b1 = q1[at]
        b2 = q2[at]
        r1, l1 = lanes(b1, -1), lanes(b1, 1)
        r2, l2 = subs(b2, -1), subs(b2, 1)
        total = c + (q0[pl.ds(xp + 2, QB)] + q0[pl.ds(xp, QB)])
        total = total + (l1 + r1)
        total = total + (l2 + r2)
        qf1[at] = b1 + r1
        qf1l[at] = b1 + l1
        qf2[at] = b2 + r2
        qf2l[at] = b2 + l2
        r = reciprocal(c, total)
        qinv[at] = r
        qmid[at] = theta * total
        w = qv0[at] * r
        qv0[at] = w
        set_rows(row_q, xp, b2[:, 3:4], b2[:, 12:13])

    q_loop(q_diag)
    set_patch(patch_q, row_q)

    def add(acc, value):
        total, lost = acc
        value = value - lost
        new = total + value
        return new, (new - total) - value

    def tree(values):
        while len(values) > 1:
            values = [sum(values[i : i + 2]) for i in range(0, len(values), 2)]
        return values[0]

    zero8 = jnp.zeros((8, 128), F32)
    none = (zero8, zero8)

    def diag_block(xp0, n, acc):
        for g in range(9):
            at = group(g)
            parts = []
            for xp in [xp0 + i for i in range(n)]:
                a2 = s2[xp, at]
                left, right = sides(a2, patch_q, xp, g)
                total = diag[xp, at]
                inside = total < 0.5 * OUTSIDE
                total = total + (left + right)
                r = jnp.where(inside, 1.0 / total, 0.0)
                b = rhs[xp, at]
                w = b * r
                inv[xp, at] = r
                mid[xp, at] = jnp.where(inside, theta * total, 0.0)
                put(v0, xp, g, w)
                f2[xp, at] = a2 + right
                f2l[xp, at] = a2 + left
                parts.append(b * w)
            if acc is not None and g < 8:
                acc = add(acc, tree(parts))
        return acc

    nu0 = blocks(diag_block, 3, none)

    def apply(v, w, qv, qw, extra, last):
        def q_first(xp):
            at = pl.ds(xp + 1, QB)
            x = qv[at]
            p4[at] = q4[at] * x
            p5[at] = q5[at] * x
            if not last:
                right, left = lanes(x, -1), lanes(x, 1)
                qdy[at] = right - left
                p3[at] = q3[at] * x
                r = qf2[at] * subs(x, -1) + qf2l[at] * subs(x, 1)
                r = r + (qf1[at] * right + qf1l[at] * left)
                qw[at] = r - qmid[at] * x

        q_loop(q_first)

        def q_second(xp):
            at, nx, pr = pl.ds(xp + 1, QB), pl.ds(xp + 2, QB), pl.ds(xp, QB)
            xa, x5 = qv[nx], p5[at]
            if not last:
                xb = qv[pr]
                dx = xa - xb
                dx4 = p4[nx] - p4[pr]
                y = qdy[at]
            x = qv[at]
            if last:
                q = p4[nx] + lanes(x5, -1)
                e, ex, eq = (t[:, :8] - t[:, 8:] for t in (x, xa, q))
                ey = pltpu.roll(e, 127, 2)
            else:
                q = dx4 + (lanes(x5, -1) - lanes(x5, 1))
                e, ex, ey, eq = (t[:, :8] - t[:, 8:] for t in (x, dx, y, q))

            def turn(t, step):
                return pltpu.roll(t, step % 8, 1)

            b4, b5 = q4[at], q5[at]
            first = -(b4[:, :8] * turn(ex, 1) + b5[:, :8] * turn(ey, 1)) - turn(eq, 1)
            if not last:
                first = first + qf2l[at][:, :8] * turn(e, 1)
            final = qf2[at][:, 8:] * turn(e, -1) + b4[:, 8:] * turn(ex, -1)
            final = final + b5[:, 8:] * turn(ey, -1) + turn(eq, -1)
            set_rows(row_q, xp, first[:, 4:5], -final[:, 3:4])
            if not last:
                b0 = q0[at]
                t = (p3[nx] - p3[pr]) + (subs(x5, -1) - subs(x5, 1))
                r = qw[at] + (b0 + q0[nx]) * xa + (b0 + q0[pr]) * xb
                r = r + (lanes(t, -1) - lanes(t, 1))
                r = r + q3[at] * (qdy[nx] - qdy[pr])
                r = r + b4 * (subs(dx, -1) - subs(dx, 1))
                r = r + b5 * (subs(y, -1) - subs(y, 1))
                r = r + (subs(dx4, -1) - subs(dx4, 1))
                qw[at] = r * qinv[at]

        q_loop(q_second)
        set_patch(patch_q, row_q)

        def first(g, xps):
            at = group(g)
            for xp in xps:
                x = v[xp, at]
                left, right = pltpu.roll(x, 1, 1), pltpu.roll(x, 127, 1)
                put(dz, xp, g, right - left)
                if last:
                    ac[xp, at] = f2[xp, at] * right
                else:
                    ac[xp, at] = f2[xp, at] * right + f2l[xp, at] * left
                put(u3, xp, g, s3[xp, at] * x)
                u4[xp, at] = s4[xp, at] * x
                put(u5, xp, g, s5[xp, at] * x)

        def second_block(xp0, n, acc, then=None):
            def start(g):
                at, nxt, prv = group(g), pl.ds(9 + 8 * g, 8), pl.ds(7 + 8 * g, 8)
                a4 = [u4[xp0 - 1 + i, at] for i in range(n + 2)]
                out = []
                for i in range(n):
                    xp = xp0 + i
                    if last:
                        q = a4[i + 2] + u5[xp, nxt]
                    else:
                        q = (a4[i + 2] - a4[i]) + (u5[xp, nxt] - u5[xp, prv])
                    p = pltpu.roll(patch_q[at], 127 - 2 * xp, 1)
                    p = jnp.where((ln == 0) | (ln == 127), p, 0.0)
                    out.append((pltpu.roll(q, 127, 1) - pltpu.roll(q, 1, 1)) + p)
                return out

            def finish_half(g, qs, acc):
                at, nxt, prv = group(g), pl.ds(9 + 8 * g, 8), pl.ds(7 + 8 * g, 8)
                dots = []
                for i in range(n):
                    xp = xp0 + i
                    x = v[xp, at]
                    r = ac[xp, at] - (0.5 * mid[xp, at]) * x
                    r = r + (f0[xp, at] * v[xp + 1, at] + f1[xp, at] * v[xp, nxt])
                    r = r + s3[xp, at] * (v[xp + 1, nxt] - v[xp + 1, prv])
                    r = r + (u3[xp + 1, nxt] - u3[xp + 1, prv])
                    r = r + (s4[xp, at] * dz[xp + 1, at] + s5[xp, at] * dz[xp, nxt])
                    dots.append((2.0 * x) * (r + qs[i]))
                return add(acc[0], tree(dots)), acc[1]

            def finish(g, qs, acc):
                if last:
                    return finish_half(g, qs, acc)
                at, nxt, prv = group(g), pl.ds(9 + 8 * g, 8), pl.ds(7 + 8 * g, 8)
                vh = [v[xp0 - 1 + i, at] for i in range(n + 2)]
                vn = [v[xp0 - 1 + i, nxt] for i in range(n + 2)]
                vp = [v[xp0 - 1 + i, prv] for i in range(n + 2)]
                un = [u3[xp0 - 1 + i, nxt] for i in range(n + 2)]
                up = [u3[xp0 - 1 + i, prv] for i in range(n + 2)]
                zh = [dz[xp0 - 1 + i, at] for i in range(n + 2)]
                fx = [f0[xp0 - 1 + i, at] for i in range(n + 1)]
                dots, norms = [], []
                for i in range(n):
                    xp = xp0 + i
                    x = vh[i + 1]
                    r = ac[xp, at] - mid[xp, at] * x
                    r = r + (fx[i + 1] * vh[i + 2] + fx[i] * vh[i])
                    r = r + (f1[xp, at] * vn[i + 1] + f1[xp, prv] * vp[i + 1])
                    r = r + s3[xp, at] * ((vn[i + 2] - vn[i]) - (vp[i + 2] - vp[i]))
                    r = r + ((un[i + 2] - un[i]) - (up[i + 2] - up[i]))
                    r = r + s4[xp, at] * (zh[i + 2] - zh[i])
                    r = r + s5[xp, at] * (dz[xp, nxt] - dz[xp, prv])
                    r = r + qs[i]
                    dots.append(x * r)
                    out = r * inv[xp, at]
                    put(w, xp, g, out)
                    norms.append(out * r)
                if acc is None or g == 8:
                    return acc
                return add(acc[0], tree(dots)), add(acc[1], tree(norms))

            count = 8 if last else 9
            ahead = 2
            pending = [start(g) for g in range(ahead)]
            for g in range(9):
                if g + ahead < count:
                    pending.append(start(g + ahead))
                if then is not None:
                    first(g, [then + i for i in range(4)])
                if g < count:
                    acc = finish(g, pending.pop(0), acc)
            return acc

        def lead(i, carry):
            for g in range(9):
                first(g, [4 * i + 1 + k for k in range(4)])
            return carry

        lax.fori_loop(0, 2, lead, 0)
        out = lax.fori_loop(
            1,
            1 + NX // 4,
            lambda i, acc: second_block(4 * i, 4, acc, 4 * i + 5),
            (none, none),
        )
        if extra:
            lax.fori_loop(
                0,
                2,
                lambda i, c: second_block(4 - extra + (32 + extra) * i, extra, None) or c,
                0,
            )
        return out

    nu1, nu2 = apply(v0, v1, qv0, qv1, 2, False)
    nu3, nu4 = apply(v1, v2, qv1, qv2, 1, False)
    nu5, _ = apply(v2, None, qv2, None, 0, True)

    def store(x, carry):
        w0o[x] = v0[x + 4, OWN]
        w1o[x] = v1[x + 4, OWN]
        w2o[x] = v2[x + 4, OWN]
        return carry

    lax.fori_loop(0, NX, store, 0)
    line = jnp.zeros((1, 128), F32)
    at = iota((1, 128), 1)
    line = jnp.where(at == 6, theta, line)
    for k, (nu, _) in enumerate((nu0, nu1, nu2, nu3, nu4, nu5)):
        part = jnp.sum(jnp.sum(nu, axis=0, keepdims=True), axis=1, keepdims=True)
        line = jnp.where(at == k, part, line)
    mom[...] = jnp.broadcast_to(line, mom.shape)


def combine(mom, w0, w1, w2, out):
    total = jnp.sum(mom[...], axis=0, keepdims=True)
    at = iota((1, 128), 1)
    m = [jnp.sum(jnp.where(at == k, total, 0.0), axis=1, keepdims=True) for k in range(7)]
    rest = 1.0 - m[6] * (1.0 / mom.shape[0])
    a = [rest * m[k] - m[k + 1] for k in range(5)]
    tiny = 1e-7

    def ratio(p, q, limit):
        ok = q > limit
        return jnp.where(ok, p / jnp.where(ok, q, 1.0), 0.0)

    l10 = a[1] / a[0]
    l20 = a[2] / a[0]
    d1 = a[2] - l10 * a[1]
    e12 = a[3] - l10 * a[2]
    g1 = m[1] - l10 * m[0]
    l21 = ratio(e12, d1, tiny * a[2])
    d2 = a[4] - l20 * a[2] - l21 * e12
    g2 = m[2] - l20 * m[0] - l21 * g1
    c2 = ratio(g2, d2, tiny * a[4])
    c1 = ratio(g1, d1, tiny * a[2]) - l21 * c2
    c0 = (m[0] - a[1] * c1 - a[2] * c2) / a[0]

    def plane(x, carry):
        out[x] = c0 * w0[x] + c1 * w1[x] + c2 * w2[x]
        return carry

    lax.fori_loop(0, NX, plane, 0)


def vmem():
    return pl.BlockSpec(memory_space=pltpu.VMEM)


def pack_planes(lab_head, lab_tail, b_head, b_tail, up, down):
    up[pl.ds(0, 3)] = b_head[...]
    up[pl.ds(3, 4)] = lab_head[...].astype(F32)
    down[pl.ds(0, 3)] = b_tail[...]
    down[pl.ds(3, 4)] = lab_tail[...].astype(F32)


def local(labels, conductivity, right_side):
    packet = jax.ShapeDtypeStruct((7, NY, NZ), F32)
    block = jax.ShapeDtypeStruct((NX, NY, NZ), F32)
    xu_own, xl_own = call(pack_planes, 4, [packet] * 2, 4)(
        labels[:4], labels[NX - 4 :], right_side[:3], right_side[NX - 3 :]
    )
    xu = ring(xu_own, "gx", -1)
    xl = ring(xl_own, "gx", 1)

    packet = jax.ShapeDtypeStruct((3, NY, 128), F32)
    lab_part, b_part = pl.pallas_call(
        pack_own,
        in_specs=[vmem()] * 2,
        out_specs=[vmem()] * 2,
        out_shape=[packet] * 2,
        compiler_params=pltpu.CompilerParams(vmem_limit_bytes=4 * 2**20),
        cost_estimate=pl.CostEstimate(flops=4 * 10**6, bytes_accessed=0, transcendentals=0),
        name="pack_own",
    )(labels, right_side)

    packet = jax.ShapeDtypeStruct((NX + 8, 8, 128), F32)
    yu_own, yd_own = call(pack_rows, 6, [packet] * 2, 4)(
        labels[:, :8], labels[:, NY - 8 :], right_side[:, :8], right_side[:, NY - 8 :], xu, xl
    )
    yu = ring(yu_own, "gy", -1)
    yd = ring(yd_own, "gy", 1)

    packet = jax.ShapeDtypeStruct((3, 80, 128), F32)
    zu_own, zd_own = call(pack_lanes, 6, [packet] * 2, 4)(lab_part, b_part, xu, xl, yu, yd)
    zu = ring(zu_own, "gz", -1)
    zd = ring(zd_own, "gz", 1)

    square = pltpu.VMEM((128, 128), F32)
    patch = pltpu.VMEM((80, 128), F32)
    main = (XP, RW, 128)
    tables = pl.pallas_call(
        faces,
        in_specs=[pl.BlockSpec(memory_space=pltpu.SMEM)] + [vmem()] * 6,
        out_specs=[vmem()] * 8,
        out_shape=[jax.ShapeDtypeStruct(main, F32)] * 8,
        scratch_shapes=[pltpu.VMEM(main, F32)] * 2,
        compiler_params=pltpu.CompilerParams(vmem_limit_bytes=5 * 2**20),
        cost_estimate=pl.CostEstimate(flops=8 * 10**6, bytes_accessed=0, transcendentals=0),
        name="faces",
    )(conductivity, labels, right_side, xu, xl, yu, yd)
    w0, w1, w2, mom = pl.pallas_call(
        sweeps,
        in_specs=[pl.BlockSpec(memory_space=pltpu.SMEM)] + [vmem()] * 12,
        out_specs=[vmem()] * 4,
        out_shape=[block, block, block, jax.ShapeDtypeStruct((128, 128), F32)],
        scratch_shapes=[pltpu.VMEM(main, F32)] * 12
        + [pltpu.VMEM((XP, 16, 128), F32)] * 19
        + [square, patch, square],
        compiler_params=pltpu.CompilerParams(vmem_limit_bytes=33 * 2**20),
        name="sweeps",
    )(conductivity, *tables, zu_own, zd_own, zu, zd)
    mom = lax.all_to_all(mom, ALL, 0, 0, tiled=True)
    return call(combine, 4, block, 6)(mom, w0, w1, w2)


def call(kernel, inputs, shapes, mib):
    many = isinstance(shapes, list)
    return pl.pallas_call(
        kernel,
        in_specs=[vmem()] * inputs,
        out_specs=[vmem()] * len(shapes) if many else vmem(),
        out_shape=shapes,
        compiler_params=pltpu.CompilerParams(vmem_limit_bytes=mib * 2**20),
        name=kernel.__name__,
    )


def solution(mesh):
    spec = P("gx", "gy", "gz")
    return jax.shard_map(
        local, mesh=mesh, in_specs=(spec, P(), spec), out_specs=spec, check_vma=False
    )
```

```python
import jax
import jax.numpy as jnp
from jax import lax
from jax.experimental import pallas as pl
from jax.experimental.pallas import tpu as pltpu
from jax.sharding import PartitionSpec as P

LABELS = 8
ALL = ("gx", "gy", "gz")
NX, NY, NZ = 32, 64, 128
XP, RW = NX + 10, NY + 24
OWN = slice(8, 8 + NY)
F32 = jnp.float32


def ring(arr, axis, step):
    count = lax.axis_size(axis)
    return lax.ppermute(arr, axis, [(i, (i + step) % count) for i in range(count)])


def iota(shape, dim):
    return lax.broadcasted_iota(jnp.int32, shape, dim)


def pack_rows(lab0, lab7, b0, b7, xu, xl, up, down):
    low = iota((8, 128), 0) < 4
    head, tail = pl.ds(0, 8), pl.ds(NY - 8, 8)

    def put(xp, lab_first, lab_last, b_first, b_last):
        up[xp] = jnp.where(low, b_first, pltpu.roll(lab_first, 4, 0))
        down[xp] = jnp.where(low, pltpu.roll(lab_last, 4, 0), b_last)

    for x in range(NX):
        put(x + 4, lab0[x].astype(F32), lab7[x].astype(F32), b0[x], b7[x])
    zero = jnp.zeros((8, 128), F32)
    for k in range(4):
        bk = (xl[k - 1, head], xl[k - 1, tail]) if k else (zero, zero)
        put(k, xl[3 + k, head], xl[3 + k, tail], *bk)
        bk = (xu[k, head], xu[k, tail]) if k < 3 else (zero, zero)
        put(36 + k, xu[3 + k, head], xu[3 + k, tail], *bk)


def rows_lab(yu, yd, xp):
    low = iota((8, 128), 0) < 4
    return pltpu.roll(jnp.where(low, yd[xp], yu[xp]), 4, 0)


def rows_b(yu, yd, xp):
    low = iota((8, 128), 0) < 4
    return jnp.where(low, yu[xp], yd[xp])


def gather(lane, planes, of, g, acc):
    for xp in planes:
        if xp // 16 != g:
            continue
        k = xp % 16
        shift = (8 * k + 4) % 128
        value = of(xp)
        acc = jnp.where(lane // 8 == k, pltpu.roll(value, shift, 1) if shift else value, acc)
    return acc


def pack_own(lab, b, lab_part, b_part):
    lane = iota((8, 128), 1)
    zero = jnp.zeros((8, 128), F32)

    def rows(rg, carry):
        at = pl.ds(pl.multiple_of(8 * rg, 8), 8)
        own = range(4, NX + 4)
        for g in range(3):
            lab_part[g, at] = gather(lane, own, lambda xp: lab[xp - 4, at].astype(F32), g, zero)
            b_part[g, at] = gather(lane, own, lambda xp: b[xp - 4, at], g, zero)
        return carry

    lax.fori_loop(0, NY // 8, rows, 0)


def pack_lanes(lab_part, b_part, xu, xl, yu, yd, up, down):
    lane = iota((8, 128), 1)
    first = lane % 8 < 4
    zero = jnp.zeros((8, 128), F32)

    def send(g, at, lab, b):
        down[g, at] = jnp.where(first, lab, pltpu.roll(b, 4, 1))
        up[g, at] = jnp.where(first, pltpu.roll(b, 124, 1), lab)

    everything = range(NX + 8)
    beside = [xp for xp in everything if xp < 4 or xp >= NX + 4]
    for g in range(3):
        lab = gather(lane, everything, lambda xp: rows_lab(yu, yd, xp), g, zero)
        b = gather(lane, everything, lambda xp: rows_b(yu, yd, xp), g, zero)
        send(g, pl.ds(0, 8), lab, b)
        send(g, pl.ds(72, 8), lab, b)
        for rg in range(NY // 8):
            at = pl.ds(8 * rg, 8)

            def lab_of(xp):
                return xl[3 + xp, at] if xp < 4 else xu[xp - 33, at]

            def b_of(xp):
                if xp < 4:
                    return xl[xp - 1, at] if xp else zero
                return xu[xp - 36, at] if xp < 39 else zero

            lab = gather(lane, beside, lab_of, g, lab_part[g, at])
            b = gather(lane, beside, b_of, g, b_part[g, at])
            send(g, group(rg), lab, b)


def group(g):
    return pl.ds(8 + 8 * g, 8)


def grid_flags():
    first, last = [], []
    for axis in ALL:
        at = lax.axis_index(axis)
        first.append((at > 0).astype(F32))
        last.append((at < lax.axis_size(axis) - 1).astype(F32))
    return first, last


def entries_of(cond):
    sub8 = iota((8, 128), 0)
    tables = []
    for c in range(7):
        t = jnp.zeros((8, 128), F32)
        scale = 0.5 if c < 3 else (0.25 if c < 6 else 1.0)
        for l in range(LABELS):
            t = jnp.where(sub8 == l, cond[c, l] * scale, t)
        tables.append(t)

    def look(c, idx):
        return jnp.take_along_axis(tables[c], idx, axis=0, mode="promise_in_bounds")

    def entries(idx, on):
        vals = [look(c, idx) for c in range(7)]
        if on is not None:
            vals = [v * on for v in vals]
        centre = vals[6] + 2.0 * (vals[0] + vals[1] + vals[2])
        return vals[:6], centre

    return entries


def put(ref, xp, g, value):
    ref[xp, group(g)] = value
    if g == 8:
        ref[xp, pl.ds(0, 8)] = value
    if g == 0:
        ref[xp, pl.ds(80, 8)] = value


def blocks(body, extra, sums):
    if extra:
        lax.fori_loop(
            0, 2, lambda i, c: body(4 - extra + (32 + extra) * i, extra, None) or c, 0
        )
    return lax.fori_loop(0, NX // 4, lambda i, acc: body(4 * i + 4, 4, acc), sums)


OUTSIDE = 1e30


def faces(cond, lab, b, xu, xl, yu, yd, f0, f1, diag, s2, s3, s4, s5, v0, s0, s1):
    sig = (s0, s1, s2, s3, s4, s5)
    (not_first_x, not_first_y, _), (not_last_x, not_last_y, _) = grid_flags()
    entries = entries_of(cond)
    sub8 = iota((8, 128), 0)
    row_on = jnp.where(sub8 < 4, not_last_y, not_first_y)

    def table_plane(xp, labels_of, b_of, on):
        for g in range(9):
            if g < 8:
                vals, centre = entries(labels_of(g), on)
                v0[xp, group(g)] = b_of(g)
            else:
                vals, centre = entries(
                    rows_lab(yu, yd, xp).astype(jnp.int32),
                    row_on if on is None else row_on * on,
                )
                v0[xp, group(g)] = rows_b(yu, yd, xp)
            for c in range(6):
                if c == 1:
                    put(s1, xp, g, vals[1])
                else:
                    sig[c][xp, group(g)] = vals[c]
            diag[xp, group(g)] = centre

    def own_plane(x, carry):
        table_plane(
            x + 4, lambda g: lab[x, pl.ds(8 * g, 8)], lambda g: b[x, pl.ds(8 * g, 8)], None
        )
        return carry

    lax.fori_loop(0, NX, own_plane, 0)

    def low_plane(k, carry):
        table_plane(
            k,
            lambda g: xl[3 + k, pl.ds(8 * g, 8)].astype(jnp.int32),
            lambda g: xl[jnp.maximum(k - 1, 0), pl.ds(8 * g, 8)],
            not_first_x,
        )
        return carry

    def high_plane(k, carry):
        table_plane(
            36 + k,
            lambda g: xu[3 + k, pl.ds(8 * g, 8)].astype(jnp.int32),
            lambda g: xu[jnp.minimum(k, 2), pl.ds(8 * g, 8)],
            not_last_x,
        )
        return carry

    lax.fori_loop(0, 4, low_plane, 0)
    lax.fori_loop(0, 4, high_plane, 0)

    def sums(xp0, n, acc):
        for g in range(9):
            at, nxt, prv = group(g), pl.ds(9 + 8 * g, 8), pl.ds(7 + 8 * g, 8)
            across = [s0[xp0 - 1 + i, at] for i in range(n + 2)]
            for i in range(n):
                xp = xp0 + i
                c = diag[xp, at]
                up = s1[xp, nxt]
                total = c + (across[i + 2] + across[i]) + (up + s1[xp, prv])
                diag[xp, at] = jnp.where(c > 0, total, OUTSIDE)
                f0[xp, at] = across[i + 1] + across[i + 2]
                put(f1, xp, g, s1[xp, at] + up)
        return acc

    blocks(sums, 3, 0)


def sweeps(
    cond, f0, f1, diag, s2, s3, s4, s5, rhs, zu_own, zd_own, zu, zd,
    w0o, w1o, w2o, mom,
    f2, f2l, inv, mid, v0, v1, v2, dz, ac, u3, u4, u5,
    q0, q1, q2, q3, q4, q5, qf1, qf1l, qf2, qf2l, qinv, qmid, qv0, qv1, qv2,
    qdy, p3, p4, p5,
    wide, patch_q, row_q,
):
    qsig = (q0, q1, q2, q3, q4, q5)
    (not_first_x, not_first_y, not_first_z), (not_last_x, not_last_y, not_last_z) = grid_flags()
    entries = entries_of(cond)
    sub8 = iota((8, 128), 0)
    ln = iota((8, 128), 1)

    mass = sum(cond[6, l] for l in range(LABELS))
    faces = sum(cond[c, l] for c in range(3) for l in range(LABELS)) * 2.0
    theta = jnp.full((1, 128), faces, F32) / jnp.full((1, 128), faces + mass, F32)

    first = iota((80, 128), 1) % 8 < 4
    wide[...] = jnp.zeros((128, 128), F32)
    lane_on = jnp.where(ln < 8, not_first_y, jnp.where(ln >= 72, not_last_y, 1.0))
    low_on = jnp.where(sub8 < 4, not_first_z, 1.0) * lane_on
    high_on = jnp.where(sub8 < 4, 1.0, not_last_z) * lane_on

    def turned(arr):
        wide[pl.ds(0, 80)] = arr
        return wide[...].T

    for g in range(3):
        count = 16 if g < 2 else 8
        parts = (
            (0, low_on, turned(jnp.where(first, zd[g], zu_own[g])),
             turned(jnp.where(first, zu_own[g], zd[g]))),
            (8, high_on, turned(jnp.where(first, zd_own[g], zu[g])),
             turned(jnp.where(first, zu[g], zd_own[g]))),
        )
        for off, on, labs, bs in parts:
            for k in range(count):
                xp = 16 * g + k
                here = on
                if xp < 4:
                    here = on * not_first_x
                if xp >= 36:
                    here = on * not_last_x
                idx = jnp.clip(labs[8 * k : 8 * k + 8].astype(jnp.int32), 0, LABELS - 1)
                vals, centre = entries(idx, here)
                for c in range(6):
                    qsig[c][xp + 1, pl.ds(off, 8)] = vals[c]
                qinv[xp + 1, pl.ds(off, 8)] = centre
                qv0[xp + 1, pl.ds(off, 8)] = pltpu.roll(bs[8 * k : 8 * k + 8], 4, 0)

    def set_rows(ref, xp, for_first, for_last):
        for k in range(QB):
            ref[pl.ds(2 * (xp + k) + 1, 1)] = for_first[k]
            ref[pl.ds(2 * (xp + k), 1)] = for_last[k]

    def set_patch(patch, rows):
        t = rows[...].T
        patch[...] = t[:80]
        patch[pl.ds(72, 8)] = jnp.where(sub8 < 4, t[72:80], t[:8])

    def sides(value, patch, xp, g):
        p = pltpu.roll(patch[group(g)], 127 - 2 * xp, 1)
        left = jnp.where(ln == 0, p, pltpu.roll(value, 1, 1))
        right = jnp.where(ln == 127, p, pltpu.roll(value, 127, 1))
        return left, right

    QB = 40

    def q_loop(body):
        lax.fori_loop(0, (NX + 8) // QB, lambda i, c: body(QB * i) or c, 0)

    def lanes(x, step):
        return pltpu.roll(x, step % 128, 2)

    def subs(x, step):
        return pltpu.roll(x, step % 16, 1)

    row_q[...] = jnp.zeros((128, 128), F32)

    def reciprocal(centre, total):
        return jnp.where(centre > 0, 1.0 / jnp.where(centre > 0, total, 1.0), 0.0)

    def q_diag(xp):
        at = pl.ds(xp + 1, QB)
        c = qinv[at]
        b1 = q1[at]
        b2 = q2[at]
        r1, l1 = lanes(b1, -1), lanes(b1, 1)
        r2, l2 = subs(b2, -1), subs(b2, 1)
        total = c + (q0[pl.ds(xp + 2, QB)] + q0[pl.ds(xp, QB)])
        total = total + (l1 + r1)
        total = total + (l2 + r2)
        qf1[at] = b1 + r1
        qf1l[at] = b1 + l1
        qf2[at] = b2 + r2
        qf2l[at] = b2 + l2
        r = reciprocal(c, total)
        qinv[at] = r
        qmid[at] = theta * total
        w = qv0[at] * r
        qv0[at] = w
        set_rows(row_q, xp, b2[:, 3:4], b2[:, 12:13])

    q_loop(q_diag)
    set_patch(patch_q, row_q)

    def add(acc, value):
        total, lost = acc
        value = value - lost
        new = total + value
        return new, (new - total) - value

    def tree(values):
        while len(values) > 1:
            values = [sum(values[i : i + 2]) for i in range(0, len(values), 2)]
        return values[0]

    zero8 = jnp.zeros((8, 128), F32)
    none = (zero8, zero8)

    def diag_block(xp0, n, acc):
        for g in range(9):
            at = group(g)
            parts = []
            for xp in [xp0 + i for i in range(n)]:
                a2 = s2[xp, at]
                left, right = sides(a2, patch_q, xp, g)
                total = diag[xp, at]
                inside = total < 0.5 * OUTSIDE
                total = total + (left + right)
                r = jnp.where(inside, 1.0 / total, 0.0)
                b = rhs[xp, at]
                w = b * r
                inv[xp, at] = r
                mid[xp, at] = jnp.where(inside, theta * total, 0.0)
                put(v0, xp, g, w)
                f2[xp, at] = a2 + right
                f2l[xp, at] = a2 + left
                parts.append(b * w)
            if acc is not None and g < 8:
                acc = add(acc, tree(parts))
        return acc

    nu0 = blocks(diag_block, 3, none)

    def apply(v, w, qv, qw, extra, last):
        def q_first(xp):
            at = pl.ds(xp + 1, QB)
            x = qv[at]
            p4[at] = q4[at] * x
            p5[at] = q5[at] * x
            if not last:
                right, left = lanes(x, -1), lanes(x, 1)
                qdy[at] = right - left
                p3[at] = q3[at] * x
                r = qf2[at] * subs(x, -1) + qf2l[at] * subs(x, 1)
                r = r + (qf1[at] * right + qf1l[at] * left)
                qw[at] = r - qmid[at] * x

        q_loop(q_first)

        def q_second(xp):
            at, nx, pr = pl.ds(xp + 1, QB), pl.ds(xp + 2, QB), pl.ds(xp, QB)
            xa, x5 = qv[nx], p5[at]
            if not last:
                xb = qv[pr]
                dx = xa - xb
                dx4 = p4[nx] - p4[pr]
                y = qdy[at]
            x = qv[at]
            if last:
                q = p4[nx] + lanes(x5, -1)
                e, ex, eq = (t[:, :8] - t[:, 8:] for t in (x, xa, q))
                ey = pltpu.roll(e, 127, 2)
            else:
                q = dx4 + (lanes(x5, -1) - lanes(x5, 1))
                e, ex, ey, eq = (t[:, :8] - t[:, 8:] for t in (x, dx, y, q))

            def turn(t, step):
                return pltpu.roll(t, step % 8, 1)

            b4, b5 = q4[at], q5[at]
            first = -(b4[:, :8] * turn(ex, 1) + b5[:, :8] * turn(ey, 1)) - turn(eq, 1)
            if not last:
                first = first + qf2l[at][:, :8] * turn(e, 1)
            final = qf2[at][:, 8:] * turn(e, -1) + b4[:, 8:] * turn(ex, -1)
            final = final + b5[:, 8:] * turn(ey, -1) + turn(eq, -1)
            set_rows(row_q, xp, first[:, 4:5], -final[:, 3:4])
            if not last:
                b0 = q0[at]
                t = (p3[nx] - p3[pr]) + (subs(x5, -1) - subs(x5, 1))
                r = qw[at] + (b0 + q0[nx]) * xa + (b0 + q0[pr]) * xb
                r = r + (lanes(t, -1) - lanes(t, 1))
                r = r + q3[at] * (qdy[nx] - qdy[pr])
                r = r + b4 * (subs(dx, -1) - subs(dx, 1))
                r = r + b5 * (subs(y, -1) - subs(y, 1))
                r = r + (subs(dx4, -1) - subs(dx4, 1))
                qw[at] = r * qinv[at]

        q_loop(q_second)
        set_patch(patch_q, row_q)

        def first(g, xps):
            at = group(g)
            for xp in xps:
                x = v[xp, at]
                left, right = pltpu.roll(x, 1, 1), pltpu.roll(x, 127, 1)
                put(dz, xp, g, right - left)
                if last:
                    ac[xp, at] = f2[xp, at] * right
                else:
                    ac[xp, at] = f2[xp, at] * right + f2l[xp, at] * left
                put(u3, xp, g, s3[xp, at] * x)
                u4[xp, at] = s4[xp, at] * x
                put(u5, xp, g, s5[xp, at] * x)

        def second_block(xp0, n, acc, then=None):
            def start(g):
                at, nxt, prv = group(g), pl.ds(9 + 8 * g, 8), pl.ds(7 + 8 * g, 8)
                a4 = [u4[xp0 - 1 + i, at] for i in range(n + 2)]
                out = []
                for i in range(n):
                    xp = xp0 + i
                    if last:
                        q = a4[i + 2] + u5[xp, nxt]
                    else:
                        q = (a4[i + 2] - a4[i]) + (u5[xp, nxt] - u5[xp, prv])
                    p = pltpu.roll(patch_q[at], 127 - 2 * xp, 1)
                    p = jnp.where((ln == 0) | (ln == 127), p, 0.0)
                    out.append((pltpu.roll(q, 127, 1) - pltpu.roll(q, 1, 1)) + p)
                return out

            def finish_half(g, qs, acc):
                at, nxt, prv = group(g), pl.ds(9 + 8 * g, 8), pl.ds(7 + 8 * g, 8)
                dots = []
                for i in range(n):
                    xp = xp0 + i
                    x = v[xp, at]
                    r = ac[xp, at] - (0.5 * mid[xp, at]) * x
                    r = r + (f0[xp, at] * v[xp + 1, at] + f1[xp, at] * v[xp, nxt])
                    r = r + s3[xp, at] * (v[xp + 1, nxt] - v[xp + 1, prv])
                    r = r + (u3[xp + 1, nxt] - u3[xp + 1, prv])
                    r = r + (s4[xp, at] * dz[xp + 1, at] + s5[xp, at] * dz[xp, nxt])
                    dots.append((2.0 * x) * (r + qs[i]))
                return add(acc[0], tree(dots)), acc[1]

            def finish(g, qs, acc):
                if last:
                    return finish_half(g, qs, acc)
                at, nxt, prv = group(g), pl.ds(9 + 8 * g, 8), pl.ds(7 + 8 * g, 8)
                vh = [v[xp0 - 1 + i, at] for i in range(n + 2)]
                vn = [v[xp0 - 1 + i, nxt] for i in range(n + 2)]
                vp = [v[xp0 - 1 + i, prv] for i in range(n + 2)]
                un = [u3[xp0 - 1 + i, nxt] for i in range(n + 2)]
                up = [u3[xp0 - 1 + i, prv] for i in range(n + 2)]
                zh = [dz[xp0 - 1 + i, at] for i in range(n + 2)]
                fx = [f0[xp0 - 1 + i, at] for i in range(n + 1)]
                dots, norms = [], []
                for i in range(n):
                    xp = xp0 + i
                    x = vh[i + 1]
                    r = ac[xp, at] - mid[xp, at] * x
                    r = r + (fx[i + 1] * vh[i + 2] + fx[i] * vh[i])
                    r = r + (f1[xp, at] * vn[i + 1] + f1[xp, prv] * vp[i + 1])
                    r = r + s3[xp, at] * ((vn[i + 2] - vn[i]) - (vp[i + 2] - vp[i]))
                    r = r + ((un[i + 2] - un[i]) - (up[i + 2] - up[i]))
                    r = r + s4[xp, at] * (zh[i + 2] - zh[i])
                    r = r + s5[xp, at] * (dz[xp, nxt] - dz[xp, prv])
                    r = r + qs[i]
                    dots.append(x * r)
                    out = r * inv[xp, at]
                    put(w, xp, g, out)
                    norms.append(out * r)
                if acc is None or g == 8:
                    return acc
                return add(acc[0], tree(dots)), add(acc[1], tree(norms))

            count = 8 if last else 9
            ahead = 2
            pending = [start(g) for g in range(ahead)]
            for g in range(9):
                if g + ahead < count:
                    pending.append(start(g + ahead))
                if then is not None:
                    first(g, [then + i for i in range(4)])
                if g < count:
                    acc = finish(g, pending.pop(0), acc)
            return acc

        def lead(i, carry):
            for g in range(9):
                first(g, [4 * i + 1 + k for k in range(4)])
            return carry

        lax.fori_loop(0, 2, lead, 0)
        out = lax.fori_loop(
            1,
            1 + NX // 4,
            lambda i, acc: second_block(4 * i, 4, acc, 4 * i + 5),
            (none, none),
        )
        if extra:
            lax.fori_loop(
                0,
                2,
                lambda i, c: second_block(4 - extra + (32 + extra) * i, extra, None) or c,
                0,
            )
        return out

    nu1, nu2 = apply(v0, v1, qv0, qv1, 2, False)
    nu3, nu4 = apply(v1, v2, qv1, qv2, 1, False)
    nu5, _ = apply(v2, None, qv2, None, 0, True)

    def store(x, carry):
        w0o[x] = v0[x + 4, OWN]
        w1o[x] = v1[x + 4, OWN]
        w2o[x] = v2[x + 4, OWN]
        return carry

    lax.fori_loop(0, NX, store, 0)
    line = jnp.zeros((1, 128), F32)
    at = iota((1, 128), 1)
    line = jnp.where(at == 6, theta, line)
    for k, (nu, _) in enumerate((nu0, nu1, nu2, nu3, nu4, nu5)):
        part = jnp.sum(jnp.sum(nu, axis=0, keepdims=True), axis=1, keepdims=True)
        line = jnp.where(at == k, part, line)
    mom[...] = jnp.broadcast_to(line, mom.shape)


def combine(mom, w0, w1, w2, out, held, sems):
    total = jnp.sum(mom[...], axis=0, keepdims=True)
    at = iota((1, 128), 1)
    m = [jnp.sum(jnp.where(at == k, total, 0.0), axis=1, keepdims=True) for k in range(7)]
    rest = 1.0 - m[6] * (1.0 / mom.shape[0])
    a = [rest * m[k] - m[k + 1] for k in range(5)]
    tiny = 1e-7

    def ratio(p, q, limit):
        ok = q > limit
        return jnp.where(ok, p / jnp.where(ok, q, 1.0), 0.0)

    l10 = a[1] / a[0]
    l20 = a[2] / a[0]
    d1 = a[2] - l10 * a[1]
    e12 = a[3] - l10 * a[2]
    g1 = m[1] - l10 * m[0]
    l21 = ratio(e12, d1, tiny * a[2])
    d2 = a[4] - l20 * a[2] - l21 * e12
    g2 = m[2] - l20 * m[0] - l21 * g1
    c2 = ratio(g2, d2, tiny * a[4])
    c1 = ratio(g1, d1, tiny * a[2]) - l21 * c2
    c0 = (m[0] - a[1] * c1 - a[2] * c2) / a[0]

    step = NX // 4

    def send(i):
        part = pl.ds(step * i, step)
        return pltpu.make_async_copy(held.at[part], out.at[part], sems.at[i])

    for i in range(4):
        part = pl.ds(step * i, step)
        held[part] = c0 * w0[part] + c1 * w1[part] + c2 * w2[part]
        send(i).start()
    for i in range(4):
        send(i).wait()


def vmem():
    return pl.BlockSpec(memory_space=pltpu.VMEM)


def pack_planes(lab_head, lab_tail, b_head, b_tail, up, down):
    up[pl.ds(0, 3)] = b_head[...]
    up[pl.ds(3, 4)] = lab_head[...].astype(F32)
    down[pl.ds(0, 3)] = b_tail[...]
    down[pl.ds(3, 4)] = lab_tail[...].astype(F32)


def local(labels, conductivity, right_side):
    packet = jax.ShapeDtypeStruct((7, NY, NZ), F32)
    block = jax.ShapeDtypeStruct((NX, NY, NZ), F32)
    xu_own, xl_own = call(pack_planes, 4, [packet] * 2, 4)(
        labels[:4], labels[NX - 4 :], right_side[:3], right_side[NX - 3 :]
    )
    xu = ring(xu_own, "gx", -1)
    xl = ring(xl_own, "gx", 1)

    packet = jax.ShapeDtypeStruct((3, NY, 128), F32)
    lab_part, b_part = pl.pallas_call(
        pack_own,
        in_specs=[vmem()] * 2,
        out_specs=[vmem()] * 2,
        out_shape=[packet] * 2,
        compiler_params=pltpu.CompilerParams(vmem_limit_bytes=4 * 2**20),
        cost_estimate=pl.CostEstimate(flops=4 * 10**6, bytes_accessed=0, transcendentals=0),
        name="pack_own",
    )(labels, right_side)

    packet = jax.ShapeDtypeStruct((NX + 8, 8, 128), F32)
    yu_own, yd_own = call(pack_rows, 6, [packet] * 2, 4)(
        labels[:, :8], labels[:, NY - 8 :], right_side[:, :8], right_side[:, NY - 8 :], xu, xl
    )
    yu = ring(yu_own, "gy", -1)
    yd = ring(yd_own, "gy", 1)

    packet = jax.ShapeDtypeStruct((3, 80, 128), F32)
    zu_own, zd_own = call(pack_lanes, 6, [packet] * 2, 4)(lab_part, b_part, xu, xl, yu, yd)
    zu = ring(zu_own, "gz", -1)
    zd = ring(zd_own, "gz", 1)

    square = pltpu.VMEM((128, 128), F32)
    patch = pltpu.VMEM((80, 128), F32)
    main = (XP, RW, 128)
    tables = pl.pallas_call(
        faces,
        in_specs=[pl.BlockSpec(memory_space=pltpu.SMEM)] + [vmem()] * 6,
        out_specs=[vmem()] * 8,
        out_shape=[jax.ShapeDtypeStruct(main, F32)] * 8,
        scratch_shapes=[pltpu.VMEM(main, F32)] * 2,
        compiler_params=pltpu.CompilerParams(vmem_limit_bytes=5 * 2**20),
        cost_estimate=pl.CostEstimate(flops=8 * 10**6, bytes_accessed=0, transcendentals=0),
        name="faces",
    )(conductivity, labels, right_side, xu, xl, yu, yd)
    w0, w1, w2, mom = pl.pallas_call(
        sweeps,
        in_specs=[pl.BlockSpec(memory_space=pltpu.SMEM)] + [vmem()] * 12,
        out_specs=[vmem()] * 4,
        out_shape=[block, block, block, jax.ShapeDtypeStruct((128, 128), F32)],
        scratch_shapes=[pltpu.VMEM(main, F32)] * 12
        + [pltpu.VMEM((XP, 16, 128), F32)] * 19
        + [square, patch, square],
        compiler_params=pltpu.CompilerParams(vmem_limit_bytes=33 * 2**20),
        name="sweeps",
    )(conductivity, *tables, zu_own, zd_own, zu, zd)
    mom = lax.all_to_all(mom, ALL, 0, 0, tiled=True)
    return pl.pallas_call(
        combine,
        in_specs=[vmem()] * 4,
        out_specs=pl.BlockSpec(memory_space=pl.ANY),
        out_shape=block,
        scratch_shapes=[pltpu.VMEM((NX, NY, NZ), F32), pltpu.SemaphoreType.DMA((4,))],
        compiler_params=pltpu.CompilerParams(vmem_limit_bytes=6 * 2**20),
        name="combine",
    )(mom, w0, w1, w2)


def call(kernel, inputs, shapes, mib):
    many = isinstance(shapes, list)
    return pl.pallas_call(
        kernel,
        in_specs=[vmem()] * inputs,
        out_specs=[vmem()] * len(shapes) if many else vmem(),
        out_shape=shapes,
        compiler_params=pltpu.CompilerParams(vmem_limit_bytes=mib * 2**20),
        name=kernel.__name__,
    )


def solution(mesh):
    spec = P("gx", "gy", "gz")
    return jax.shard_map(
        local, mesh=mesh, in_specs=(spec, P(), spec), out_specs=spec, check_vma=False
    )
```

```python
import jax
import jax.numpy as jnp
from jax import lax
from jax.experimental import pallas as pl
from jax.experimental.pallas import tpu as pltpu
from jax.sharding import PartitionSpec as P

LABELS = 8
ALL = ("gx", "gy", "gz")
NX, NY, NZ = 32, 64, 128
XP, RW = NX + 10, NY + 24
OWN = slice(8, 8 + NY)
F32 = jnp.float32


def ring(arr, axis, step):
    count = lax.axis_size(axis)
    return lax.ppermute(arr, axis, [(i, (i + step) % count) for i in range(count)])


def iota(shape, dim):
    return lax.broadcasted_iota(jnp.int32, shape, dim)


def pack_rows(lab0, lab7, b0, b7, xu, xl, up, down):
    low = iota((8, 128), 0) < 4
    head, tail = pl.ds(0, 8), pl.ds(NY - 8, 8)

    def put(xp, lab_first, lab_last, b_first, b_last):
        up[xp] = jnp.where(low, b_first, pltpu.roll(lab_first, 4, 0))
        down[xp] = jnp.where(low, pltpu.roll(lab_last, 4, 0), b_last)

    for x in range(NX):
        put(x + 4, lab0[x].astype(F32), lab7[x].astype(F32), b0[x], b7[x])
    zero = jnp.zeros((8, 128), F32)
    for k in range(4):
        bk = (xl[k - 1, head], xl[k - 1, tail]) if k else (zero, zero)
        put(k, xl[3 + k, head], xl[3 + k, tail], *bk)
        bk = (xu[k, head], xu[k, tail]) if k < 3 else (zero, zero)
        put(36 + k, xu[3 + k, head], xu[3 + k, tail], *bk)


def rows_lab(yu, yd, xp):
    low = iota((8, 128), 0) < 4
    return pltpu.roll(jnp.where(low, yd[xp], yu[xp]), 4, 0)


def rows_b(yu, yd, xp):
    low = iota((8, 128), 0) < 4
    return jnp.where(low, yu[xp], yd[xp])


def gather(lane, planes, of, g, acc):
    for xp in planes:
        if xp // 16 != g:
            continue
        k = xp % 16
        shift = (8 * k + 4) % 128
        value = of(xp)
        acc = jnp.where(lane // 8 == k, pltpu.roll(value, shift, 1) if shift else value, acc)
    return acc


def pack_own(lab, b, lab_part, b_part):
    lane = iota((8, 128), 1)
    zero = jnp.zeros((8, 128), F32)

    def rows(rg, carry):
        at = pl.ds(pl.multiple_of(8 * rg, 8), 8)
        own = range(4, NX + 4)
        for g in range(3):
            lab_part[g, at] = gather(lane, own, lambda xp: lab[xp - 4, at].astype(F32), g, zero)
            b_part[g, at] = gather(lane, own, lambda xp: b[xp - 4, at], g, zero)
        return carry

    lax.fori_loop(0, NY // 8, rows, 0)


def pack_lanes(lab_part, b_part, xu, xl, yu, yd, up, down):
    lane = iota((8, 128), 1)
    first = lane % 8 < 4
    zero = jnp.zeros((8, 128), F32)

    def send(g, at, lab, b):
        down[g, at] = jnp.where(first, lab, pltpu.roll(b, 4, 1))
        up[g, at] = jnp.where(first, pltpu.roll(b, 124, 1), lab)

    everything = range(NX + 8)
    beside = [xp for xp in everything if xp < 4 or xp >= NX + 4]
    for g in range(3):
        lab = gather(lane, everything, lambda xp: rows_lab(yu, yd, xp), g, zero)
        b = gather(lane, everything, lambda xp: rows_b(yu, yd, xp), g, zero)
        send(g, pl.ds(0, 8), lab, b)
        send(g, pl.ds(72, 8), lab, b)
        for rg in range(NY // 8):
            at = pl.ds(8 * rg, 8)

            def lab_of(xp):
                return xl[3 + xp, at] if xp < 4 else xu[xp - 33, at]

            def b_of(xp):
                if xp < 4:
                    return xl[xp - 1, at] if xp else zero
                return xu[xp - 36, at] if xp < 39 else zero

            lab = gather(lane, beside, lab_of, g, lab_part[g, at])
            b = gather(lane, beside, b_of, g, b_part[g, at])
            send(g, group(rg), lab, b)


def group(g):
    return pl.ds(8 + 8 * g, 8)


def grid_flags():
    first, last = [], []
    for axis in ALL:
        at = lax.axis_index(axis)
        first.append((at > 0).astype(F32))
        last.append((at < lax.axis_size(axis) - 1).astype(F32))
    return first, last


def entries_of(cond):
    sub8 = iota((8, 128), 0)
    tables = []
    for c in range(7):
        t = jnp.zeros((8, 128), F32)
        scale = 0.5 if c < 3 else (0.25 if c < 6 else 1.0)
        for l in range(LABELS):
            t = jnp.where(sub8 == l, cond[c, l] * scale, t)
        tables.append(t)

    def look(c, idx):
        return jnp.take_along_axis(tables[c], idx, axis=0, mode="promise_in_bounds")

    def entries(idx, on):
        vals = [look(c, idx) for c in range(7)]
        if on is not None:
            vals = [v * on for v in vals]
        centre = vals[6] + 2.0 * (vals[0] + vals[1] + vals[2])
        return vals[:6], centre

    return entries


def put(ref, xp, g, value):
    ref[xp, group(g)] = value
    if g == 8:
        ref[xp, pl.ds(0, 8)] = value
    if g == 0:
        ref[xp, pl.ds(80, 8)] = value


def blocks(body, extra, sums):
    if extra:
        lax.fori_loop(
            0, 2, lambda i, c: body(4 - extra + (32 + extra) * i, extra, None) or c, 0
        )
    return lax.fori_loop(0, NX // 4, lambda i, acc: body(4 * i + 4, 4, acc), sums)


OUTSIDE = 1e30


def faces(cond, lab, b, xu, xl, yu, yd, f0, f1, diag, s2, s3, s4, s5, v0, s0, s1):
    sig = (s0, s1, s2, s3, s4, s5)
    (not_first_x, not_first_y, _), (not_last_x, not_last_y, _) = grid_flags()
    entries = entries_of(cond)
    sub8 = iota((8, 128), 0)
    row_on = jnp.where(sub8 < 4, not_last_y, not_first_y)

    def table_plane(xp, labels_of, b_of, on):
        for g in range(9):
            if g < 8:
                vals, centre = entries(labels_of(g), on)
                v0[xp, group(g)] = b_of(g)
            else:
                vals, centre = entries(
                    rows_lab(yu, yd, xp).astype(jnp.int32),
                    row_on if on is None else row_on * on,
                )
                v0[xp, group(g)] = rows_b(yu, yd, xp)
            for c in range(6):
                if c == 1:
                    put(s1, xp, g, vals[1])
                else:
                    sig[c][xp, group(g)] = vals[c]
            diag[xp, group(g)] = centre

    def own_plane(x, carry):
        table_plane(
            x + 4, lambda g: lab[x, pl.ds(8 * g, 8)], lambda g: b[x, pl.ds(8 * g, 8)], None
        )
        return carry

    lax.fori_loop(0, NX, own_plane, 0)

    def low_plane(k, carry):
        table_plane(
            k,
            lambda g: xl[3 + k, pl.ds(8 * g, 8)].astype(jnp.int32),
            lambda g: xl[jnp.maximum(k - 1, 0), pl.ds(8 * g, 8)],
            not_first_x,
        )
        return carry

    def high_plane(k, carry):
        table_plane(
            36 + k,
            lambda g: xu[3 + k, pl.ds(8 * g, 8)].astype(jnp.int32),
            lambda g: xu[jnp.minimum(k, 2), pl.ds(8 * g, 8)],
            not_last_x,
        )
        return carry

    lax.fori_loop(0, 4, low_plane, 0)
    lax.fori_loop(0, 4, high_plane, 0)

    def sums(xp0, n, acc):
        for g in range(9):
            at, nxt, prv = group(g), pl.ds(9 + 8 * g, 8), pl.ds(7 + 8 * g, 8)
            across = [s0[xp0 - 1 + i, at] for i in range(n + 2)]
            for i in range(n):
                xp = xp0 + i
                c = diag[xp, at]
                up = s1[xp, nxt]
                total = c + (across[i + 2] + across[i]) + (up + s1[xp, prv])
                diag[xp, at] = jnp.where(c > 0, total, OUTSIDE)
                f0[xp, at] = across[i + 1] + across[i + 2]
                put(f1, xp, g, s1[xp, at] + up)
        return acc

    blocks(sums, 3, 0)


def sweeps(
    cond, f0, f1, diag, s2, s3, s4, s5, rhs, zu_own, zd_own, zu, zd,
    w0o, w1o, w2o, mom,
    f2, f2l, inv, mid, v0, v1, v2, dz, ac, u3, u4, u5,
    q0, q1, q2, q3, q4, q5, qf1, qf1l, qf2, qf2l, qinv, qmid, qv0, qv1, qv2,
    qdy, p3, p4, p5,
    wide, patch_q, row_q,
):
    qsig = (q0, q1, q2, q3, q4, q5)
    (not_first_x, not_first_y, not_first_z), (not_last_x, not_last_y, not_last_z) = grid_flags()
    entries = entries_of(cond)
    sub8 = iota((8, 128), 0)
    ln = iota((8, 128), 1)

    mass = sum(cond[6, l] for l in range(LABELS))
    faces = sum(cond[c, l] for c in range(3) for l in range(LABELS)) * 2.0
    theta = jnp.full((1, 128), faces, F32) / jnp.full((1, 128), faces + mass, F32)

    first = iota((80, 128), 1) % 8 < 4
    wide[...] = jnp.zeros((128, 128), F32)
    lane_on = jnp.where(ln < 8, not_first_y, jnp.where(ln >= 72, not_last_y, 1.0))
    low_on = jnp.where(sub8 < 4, not_first_z, 1.0) * lane_on
    high_on = jnp.where(sub8 < 4, 1.0, not_last_z) * lane_on

    def turned(arr):
        wide[pl.ds(0, 80)] = arr
        return wide[...].T

    for g in range(3):
        count = 16 if g < 2 else 8
        parts = (
            (0, low_on, turned(jnp.where(first, zd[g], zu_own[g])),
             turned(jnp.where(first, zu_own[g], zd[g]))),
            (8, high_on, turned(jnp.where(first, zd_own[g], zu[g])),
             turned(jnp.where(first, zu[g], zd_own[g]))),
        )
        for off, on, labs, bs in parts:
            for k in range(count):
                xp = 16 * g + k
                here = on
                if xp < 4:
                    here = on * not_first_x
                if xp >= 36:
                    here = on * not_last_x
                idx = jnp.clip(labs[8 * k : 8 * k + 8].astype(jnp.int32), 0, LABELS - 1)
                vals, centre = entries(idx, here)
                for c in range(6):
                    qsig[c][xp + 1, pl.ds(off, 8)] = vals[c]
                qinv[xp + 1, pl.ds(off, 8)] = centre
                qv0[xp + 1, pl.ds(off, 8)] = pltpu.roll(bs[8 * k : 8 * k + 8], 4, 0)

    def set_rows(ref, xp, for_first, for_last):
        for k in range(QB):
            ref[pl.ds(2 * (xp + k) + 1, 1)] = for_first[k]
            ref[pl.ds(2 * (xp + k), 1)] = for_last[k]

    def set_patch(patch, rows):
        t = rows[...].T
        patch[...] = t[:80]
        patch[pl.ds(72, 8)] = jnp.where(sub8 < 4, t[72:80], t[:8])

    def sides(value, patch, xp, g):
        p = pltpu.roll(patch[group(g)], 127 - 2 * xp, 1)
        left = jnp.where(ln == 0, p, pltpu.roll(value, 1, 1))
        right = jnp.where(ln == 127, p, pltpu.roll(value, 127, 1))
        return left, right

    QB = 40

    def q_loop(body):
        lax.fori_loop(0, (NX + 8) // QB, lambda i, c: body(QB * i) or c, 0)

    def lanes(x, step):
        return pltpu.roll(x, step % 128, 2)

    def subs(x, step):
        return pltpu.roll(x, step % 16, 1)

    row_q[...] = jnp.zeros((128, 128), F32)

    def reciprocal(centre, total):
        return jnp.where(centre > 0, 1.0 / jnp.where(centre > 0, total, 1.0), 0.0)

    def q_diag(xp):
        at = pl.ds(xp + 1, QB)
        c = qinv[at]
        b1 = q1[at]
        b2 = q2[at]
        r1, l1 = lanes(b1, -1), lanes(b1, 1)
        r2, l2 = subs(b2, -1), subs(b2, 1)
        total = c + (q0[pl.ds(xp + 2, QB)] + q0[pl.ds(xp, QB)])
        total = total + (l1 + r1)
        total = total + (l2 + r2)
        qf1[at] = b1 + r1
        qf1l[at] = b1 + l1
        qf2[at] = b2 + r2
        qf2l[at] = b2 + l2
        r = reciprocal(c, total)
        qinv[at] = r
        qmid[at] = theta * total
        w = qv0[at] * r
        qv0[at] = w
        set_rows(row_q, xp, b2[:, 3:4], b2[:, 12:13])

    q_loop(q_diag)
    set_patch(patch_q, row_q)

    def add(acc, value):
        total, lost = acc
        value = value - lost
        new = total + value
        return new, (new - total) - value

    def tree(values):
        while len(values) > 1:
            values = [sum(values[i : i + 2]) for i in range(0, len(values), 2)]
        return values[0]

    zero8 = jnp.zeros((8, 128), F32)
    none = (zero8, zero8)

    def diag_block(xp0, n, acc):
        for g in range(9):
            at = group(g)
            parts = []
            for xp in [xp0 + i for i in range(n)]:
                a2 = s2[xp, at]
                left, right = sides(a2, patch_q, xp, g)
                total = diag[xp, at]
                inside = total < 0.5 * OUTSIDE
                total = total + (left + right)
                r = jnp.where(inside, 1.0 / total, 0.0)
                b = rhs[xp, at]
                w = b * r
                inv[xp, at] = r
                mid[xp, at] = jnp.where(inside, theta * total, 0.0)
                put(v0, xp, g, w)
                if acc is not None and g < 8:
                    w0o[xp - 4, pl.ds(8 * g, 8)] = w
                f2[xp, at] = a2 + right
                f2l[xp, at] = a2 + left
                parts.append(b * w)
            if acc is not None and g < 8:
                acc = add(acc, tree(parts))
        return acc

    nu0 = blocks(diag_block, 3, none)

    def apply(v, w, wo, qv, qw, extra, last):
        def q_first(xp):
            at = pl.ds(xp + 1, QB)
            x = qv[at]
            p4[at] = q4[at] * x
            p5[at] = q5[at] * x
            if not last:
                right, left = lanes(x, -1), lanes(x, 1)
                qdy[at] = right - left
                p3[at] = q3[at] * x
                r = qf2[at] * subs(x, -1) + qf2l[at] * subs(x, 1)
                r = r + (qf1[at] * right + qf1l[at] * left)
                qw[at] = r - qmid[at] * x

        q_loop(q_first)

        def q_second(xp):
            at, nx, pr = pl.ds(xp + 1, QB), pl.ds(xp + 2, QB), pl.ds(xp, QB)
            xa, x5 = qv[nx], p5[at]
            if not last:
                xb = qv[pr]
                dx = xa - xb
                dx4 = p4[nx] - p4[pr]
                y = qdy[at]
            x = qv[at]
            if last:
                q = p4[nx] + lanes(x5, -1)
                e, ex, eq = (t[:, :8] - t[:, 8:] for t in (x, xa, q))
                ey = pltpu.roll(e, 127, 2)
            else:
                q = dx4 + (lanes(x5, -1) - lanes(x5, 1))
                e, ex, ey, eq = (t[:, :8] - t[:, 8:] for t in (x, dx, y, q))

            def turn(t, step):
                return pltpu.roll(t, step % 8, 1)

            b4, b5 = q4[at], q5[at]
            first = -(b4[:, :8] * turn(ex, 1) + b5[:, :8] * turn(ey, 1)) - turn(eq, 1)
            if not last:
                first = first + qf2l[at][:, :8] * turn(e, 1)
            final = qf2[at][:, 8:] * turn(e, -1) + b4[:, 8:] * turn(ex, -1)
            final = final + b5[:, 8:] * turn(ey, -1) + turn(eq, -1)
            set_rows(row_q, xp, first[:, 4:5], -final[:, 3:4])
            if not last:
                b0 = q0[at]
                t = (p3[nx] - p3[pr]) + (subs(x5, -1) - subs(x5, 1))
                r = qw[at] + (b0 + q0[nx]) * xa + (b0 + q0[pr]) * xb
                r = r + (lanes(t, -1) - lanes(t, 1))
                r = r + q3[at] * (qdy[nx] - qdy[pr])
                r = r + b4 * (subs(dx, -1) - subs(dx, 1))
                r = r + b5 * (subs(y, -1) - subs(y, 1))
                r = r + (subs(dx4, -1) - subs(dx4, 1))
                qw[at] = r * qinv[at]

        q_loop(q_second)
        set_patch(patch_q, row_q)

        def first(g, xps):
            at = group(g)
            for xp in xps:
                x = v[xp, at]
                left, right = pltpu.roll(x, 1, 1), pltpu.roll(x, 127, 1)
                put(dz, xp, g, right - left)
                if last:
                    ac[xp, at] = f2[xp, at] * right
                else:
                    ac[xp, at] = f2[xp, at] * right + f2l[xp, at] * left
                put(u3, xp, g, s3[xp, at] * x)
                u4[xp, at] = s4[xp, at] * x
                put(u5, xp, g, s5[xp, at] * x)

        def second_block(xp0, n, acc, then=None):
            def start(g):
                at, nxt, prv = group(g), pl.ds(9 + 8 * g, 8), pl.ds(7 + 8 * g, 8)
                a4 = [u4[xp0 - 1 + i, at] for i in range(n + 2)]
                out = []
                for i in range(n):
                    xp = xp0 + i
                    if last:
                        q = a4[i + 2] + u5[xp, nxt]
                    else:
                        q = (a4[i + 2] - a4[i]) + (u5[xp, nxt] - u5[xp, prv])
                    p = pltpu.roll(patch_q[at], 127 - 2 * xp, 1)
                    p = jnp.where((ln == 0) | (ln == 127), p, 0.0)
                    out.append((pltpu.roll(q, 127, 1) - pltpu.roll(q, 1, 1)) + p)
                return out

            def finish_half(g, qs, acc):
                at, nxt, prv = group(g), pl.ds(9 + 8 * g, 8), pl.ds(7 + 8 * g, 8)
                dots = []
                for i in range(n):
                    xp = xp0 + i
                    x = v[xp, at]
                    r = ac[xp, at] - (0.5 * mid[xp, at]) * x
                    r = r + (f0[xp, at] * v[xp + 1, at] + f1[xp, at] * v[xp, nxt])
                    r = r + s3[xp, at] * (v[xp + 1, nxt] - v[xp + 1, prv])
                    r = r + (u3[xp + 1, nxt] - u3[xp + 1, prv])
                    r = r + (s4[xp, at] * dz[xp + 1, at] + s5[xp, at] * dz[xp, nxt])
                    dots.append((2.0 * x) * (r + qs[i]))
                return add(acc[0], tree(dots)), acc[1]

            def finish(g, qs, acc):
                if last:
                    return finish_half(g, qs, acc)
                at, nxt, prv = group(g), pl.ds(9 + 8 * g, 8), pl.ds(7 + 8 * g, 8)
                vh = [v[xp0 - 1 + i, at] for i in range(n + 2)]
                vn = [v[xp0 - 1 + i, nxt] for i in range(n + 2)]
                vp = [v[xp0 - 1 + i, prv] for i in range(n + 2)]
                un = [u3[xp0 - 1 + i, nxt] for i in range(n + 2)]
                up = [u3[xp0 - 1 + i, prv] for i in range(n + 2)]
                zh = [dz[xp0 - 1 + i, at] for i in range(n + 2)]
                fx = [f0[xp0 - 1 + i, at] for i in range(n + 1)]
                dots, norms = [], []
                for i in range(n):
                    xp = xp0 + i
                    x = vh[i + 1]
                    r = ac[xp, at] - mid[xp, at] * x
                    r = r + (fx[i + 1] * vh[i + 2] + fx[i] * vh[i])
                    r = r + (f1[xp, at] * vn[i + 1] + f1[xp, prv] * vp[i + 1])
                    r = r + s3[xp, at] * ((vn[i + 2] - vn[i]) - (vp[i + 2] - vp[i]))
                    r = r + ((un[i + 2] - un[i]) - (up[i + 2] - up[i]))
                    r = r + s4[xp, at] * (zh[i + 2] - zh[i])
                    r = r + s5[xp, at] * (dz[xp, nxt] - dz[xp, prv])
                    r = r + qs[i]
                    dots.append(x * r)
                    out = r * inv[xp, at]
                    put(w, xp, g, out)
                    if acc is not None and g < 8:
                        wo[xp - 4, pl.ds(8 * g, 8)] = out
                    norms.append(out * r)
                if acc is None or g == 8:
                    return acc
                return add(acc[0], tree(dots)), add(acc[1], tree(norms))

            count = 8 if last else 9
            ahead = 2
            pending = [start(g) for g in range(ahead)]
            for g in range(9):
                if g + ahead < count:
                    pending.append(start(g + ahead))
                if then is not None:
                    first(g, [then + i for i in range(4)])
                if g < count:
                    acc = finish(g, pending.pop(0), acc)
            return acc

        def lead(i, carry):
            for g in range(9):
                first(g, [4 * i + 1 + k for k in range(4)])
            return carry

        lax.fori_loop(0, 2, lead, 0)
        out = lax.fori_loop(
            1,
            1 + NX // 4,
            lambda i, acc: second_block(4 * i, 4, acc, 4 * i + 5),
            (none, none),
        )
        if extra:
            lax.fori_loop(
                0,
                2,
                lambda i, c: second_block(4 - extra + (32 + extra) * i, extra, None) or c,
                0,
            )
        return out

    nu1, nu2 = apply(v0, v1, w1o, qv0, qv1, 2, False)
    nu3, nu4 = apply(v1, v2, w2o, qv1, qv2, 1, False)
    nu5, _ = apply(v2, None, None, qv2, None, 0, True)

    line = jnp.zeros((1, 128), F32)
    at = iota((1, 128), 1)
    line = jnp.where(at == 6, theta, line)
    for k, (nu, _) in enumerate((nu0, nu1, nu2, nu3, nu4, nu5)):
        part = jnp.sum(jnp.sum(nu, axis=0, keepdims=True), axis=1, keepdims=True)
        line = jnp.where(at == k, part, line)
    mom[...] = jnp.broadcast_to(line, mom.shape)


def combine(mom, w0, w1, w2, out):
    total = jnp.sum(mom[...], axis=0, keepdims=True)
    at = iota((1, 128), 1)
    m = [jnp.sum(jnp.where(at == k, total, 0.0), axis=1, keepdims=True) for k in range(7)]
    rest = 1.0 - m[6] * (1.0 / mom.shape[0])
    a = [rest * m[k] - m[k + 1] for k in range(5)]
    tiny = 1e-7

    def ratio(p, q, limit):
        ok = q > limit
        return jnp.where(ok, p / jnp.where(ok, q, 1.0), 0.0)

    l10 = a[1] / a[0]
    l20 = a[2] / a[0]
    d1 = a[2] - l10 * a[1]
    e12 = a[3] - l10 * a[2]
    g1 = m[1] - l10 * m[0]
    l21 = ratio(e12, d1, tiny * a[2])
    d2 = a[4] - l20 * a[2] - l21 * e12
    g2 = m[2] - l20 * m[0] - l21 * g1
    c2 = ratio(g2, d2, tiny * a[4])
    c1 = ratio(g1, d1, tiny * a[2]) - l21 * c2
    c0 = (m[0] - a[1] * c1 - a[2] * c2) / a[0]

    def plane(x, carry):
        out[x] = c0 * w0[x] + c1 * w1[x] + c2 * w2[x]
        return carry

    lax.fori_loop(0, NX, plane, 0)


def vmem():
    return pl.BlockSpec(memory_space=pltpu.VMEM)


def pack_planes(lab_head, lab_tail, b_head, b_tail, up, down):
    up[pl.ds(0, 3)] = b_head[...]
    up[pl.ds(3, 4)] = lab_head[...].astype(F32)
    down[pl.ds(0, 3)] = b_tail[...]
    down[pl.ds(3, 4)] = lab_tail[...].astype(F32)


def local(labels, conductivity, right_side):
    packet = jax.ShapeDtypeStruct((7, NY, NZ), F32)
    block = jax.ShapeDtypeStruct((NX, NY, NZ), F32)
    xu_own, xl_own = call(pack_planes, 4, [packet] * 2, 4)(
        labels[:4], labels[NX - 4 :], right_side[:3], right_side[NX - 3 :]
    )
    xu = ring(xu_own, "gx", -1)
    xl = ring(xl_own, "gx", 1)

    packet = jax.ShapeDtypeStruct((3, NY, 128), F32)
    lab_part, b_part = pl.pallas_call(
        pack_own,
        in_specs=[vmem()] * 2,
        out_specs=[vmem()] * 2,
        out_shape=[packet] * 2,
        compiler_params=pltpu.CompilerParams(vmem_limit_bytes=4 * 2**20),
        cost_estimate=pl.CostEstimate(flops=4 * 10**6, bytes_accessed=0, transcendentals=0),
        name="pack_own",
    )(labels, right_side)

    packet = jax.ShapeDtypeStruct((NX + 8, 8, 128), F32)
    yu_own, yd_own = call(pack_rows, 6, [packet] * 2, 4)(
        labels[:, :8], labels[:, NY - 8 :], right_side[:, :8], right_side[:, NY - 8 :], xu, xl
    )
    yu = ring(yu_own, "gy", -1)
    yd = ring(yd_own, "gy", 1)

    packet = jax.ShapeDtypeStruct((3, 80, 128), F32)
    zu_own, zd_own = call(pack_lanes, 6, [packet] * 2, 4)(lab_part, b_part, xu, xl, yu, yd)
    zu = ring(zu_own, "gz", -1)
    zd = ring(zd_own, "gz", 1)

    square = pltpu.VMEM((128, 128), F32)
    patch = pltpu.VMEM((80, 128), F32)
    main = (XP, RW, 128)
    tables = pl.pallas_call(
        faces,
        in_specs=[pl.BlockSpec(memory_space=pltpu.SMEM)] + [vmem()] * 6,
        out_specs=[vmem()] * 8,
        out_shape=[jax.ShapeDtypeStruct(main, F32)] * 8,
        scratch_shapes=[pltpu.VMEM(main, F32)] * 2,
        compiler_params=pltpu.CompilerParams(vmem_limit_bytes=5 * 2**20),
        cost_estimate=pl.CostEstimate(flops=8 * 10**6, bytes_accessed=0, transcendentals=0),
        name="faces",
    )(conductivity, labels, right_side, xu, xl, yu, yd)
    w0, w1, w2, mom = pl.pallas_call(
        sweeps,
        in_specs=[pl.BlockSpec(memory_space=pltpu.SMEM)] + [vmem()] * 12,
        out_specs=[vmem()] * 4,
        out_shape=[block, block, block, jax.ShapeDtypeStruct((128, 128), F32)],
        scratch_shapes=[pltpu.VMEM(main, F32)] * 12
        + [pltpu.VMEM((XP, 16, 128), F32)] * 19
        + [square, patch, square],
        compiler_params=pltpu.CompilerParams(vmem_limit_bytes=33 * 2**20),
        name="sweeps",
    )(conductivity, *tables, zu_own, zd_own, zu, zd)
    mom = lax.all_to_all(mom, ALL, 0, 0, tiled=True)
    return call(combine, 4, block, 6)(mom, w0, w1, w2)


def call(kernel, inputs, shapes, mib):
    many = isinstance(shapes, list)
    return pl.pallas_call(
        kernel,
        in_specs=[vmem()] * inputs,
        out_specs=[vmem()] * len(shapes) if many else vmem(),
        out_shape=shapes,
        compiler_params=pltpu.CompilerParams(vmem_limit_bytes=mib * 2**20),
        name=kernel.__name__,
    )


def solution(mesh):
    spec = P("gx", "gy", "gz")
    return jax.shard_map(
        local, mesh=mesh, in_specs=(spec, P(), spec), out_specs=spec, check_vma=False
    )
```
